512 devices in a mesh: replica: 64 (over z, x, core), spatial: 8 (over y).
Axes of the slice: x: 4, y: 8, z: 8, core: 2. Of those that a mesh axis runs over, the one named last changes fastest.
Arguments:
- grads: bfloat16 [64, 8, 852992], P('replica', 'spatial'), may hold values from -16 to 16
- master: float32 [852992], P(('replica', 'spatial')), may hold values from -0.06 to 0.06
- velocity: float32 [852992], P(('replica', 'spatial')), may hold values from -0.3 to 0.3
- layer_offsets: int32 [6], replicated, may hold values from 0 to 852736, as said below
- layer_sizes: int32 [6], replicated, may hold values from 256 to 589824
- lars_skip: int32 [6], replicated, may hold values from 0 to 1
Outputs:
- new_weights: bfloat16 [852992], replicated
- new_master: float32 [852992], P(('replica', 'spatial'))
- new_velocity: float32 [852992], P(('replica', 'spatial'))
The draws below stay inside these ranges and needn't reach their ends.
Inputs may be any that keep to these rules, and one draw needn't show every extreme that they name: layer_offsets, layer_sizes and lars_skip describe the six tensors (a 256 x 1024 convolution, a 256 x 256 x 9 convolution, and two gains and two shifts of 256 entries) laid end to end in some order without gaps, the last of them always a gain or a shift; lars_skip is 1 exactly for the gains and shifts.
All inputs are finite; a program needn't handle non-finite values.
Results may differ from the reference program's by a relative error of at most 0.001.
Values may be sent and summed in bfloat16 or wider, within the bound.
No kernel may reach another device: no remote copies, remote signals or barrier semaphores. Data moves between devices by JAX's collectives and lax.ppermute only.
A program may use at most 64 MiB of HBM per device.

```python
import jax
import jax.numpy as jnp
from jax import lax

CIN = 1024
MID = 256
KSQ = 9
LAYERS = 6
PARAMS = 852992
N_REPLICA = 64
N_SPATIAL = 8


def layout_tables(key):
    scores = jax.random.permutation(jax.random.fold_in(key, 71), LAYERS).astype(jnp.int32)
    small_list = jnp.array([1, 2, 4, 5], jnp.int32)
    pick = jax.random.randint(jax.random.fold_in(key, 73), (), 0, 4)
    chosen = small_list[pick]
    scores = jnp.where(jnp.arange(LAYERS, dtype=jnp.int32) == chosen, LAYERS, scores)
    order = jnp.argsort(scores, stable=True)
    base_sizes = jnp.array([MID * CIN, MID, MID, MID * MID * KSQ, MID, MID], jnp.int32)
    base_skip = jnp.array([0, 1, 1, 0, 1, 1], jnp.int32)
    sizes = base_sizes[order]
    offsets = jnp.cumsum(sizes) - sizes
    return (offsets.astype(jnp.int32), sizes.astype(jnp.int32), base_skip[order])


def draw_layer_offsets(key, part):
    return layout_tables(key)[0]


def draw_layer_sizes(key, part):
    return layout_tables(key)[1]


def draw_lars_skip(key, part):
    return layout_tables(key)[2]


def raised(values, rng, source, target, blocks, factor):
    owner, partner = [(jnp.arange(values.shape[dim]) // (values.shape[dim] // blocks)).reshape([-1 if axis == dim else 1 for axis in range(values.ndim)]) for dim in (source, target)]
    chosen = jax.random.permutation(rng, blocks)[partner]
    strong = (owner == chosen) | (owner == (partner + blocks // 2) % blocks)
    return jnp.where(strong, factor * values, values)


def levels(stream_key, extent, split, smallest, high):
    loudness, own = 1.0, jax.random.fold_in(stream_key, 6)
    for axis_at, blocks in split:
        heights = jnp.exp(jax.random.uniform(jax.random.fold_in(own, axis_at), (blocks,), jnp.float32, smallest / len(split), high / len(split)))
        loudness = loudness * jnp.repeat(heights, extent[axis_at] // blocks).reshape([-1 if axis == axis_at else 1 for axis in range(len(extent))])
    return loudness


def gaussian(stream_key, extent, scale, limit, cuts=(), held_as=jnp.bfloat16):
    values = jax.random.normal(stream_key, extent, jnp.float32) * scale
    if len(cuts) > 0:
        values = levels(stream_key, extent, cuts, -0.22, 0.18) * values
    return jnp.clip(values, min=-limit, max=limit).astype(held_as)


def gaussian_with(key, shape, scale, bound, pieces, heavy, kind=jnp.bfloat16):
    values = scale * jax.random.normal(key, shape, jnp.float32)
    if pieces:
        values = values * levels(key, shape, pieces, -0.22, 0.18)
    return jnp.clip(raised(values, jax.random.fold_in(key, 3), *heavy), -bound, bound).astype(kind)


def setup_inputs(seed: int = 0) -> dict:
    keys = jax.random.split(jax.random.key(seed), 7)
    grads = gaussian_with(keys[0], (N_REPLICA, N_SPATIAL, PARAMS), 1.0, 16.0, ((0, 64), (1, 8)), (0, 2, 64, 4.0))
    master = jnp.clip(jax.random.uniform(keys[1], (PARAMS,), jnp.float32, -0.06, 0.06) * levels(keys[1], (PARAMS,), ((0, 512),), -0.4, 0.0), -0.06, 0.06)
    velocity = gaussian(keys[2], (PARAMS,), 0.05, 0.3, ((0, 512),), jnp.float32)
    layer_offsets = draw_layer_offsets(jax.random.fold_in(keys[6], 71), 0)
    layer_sizes = draw_layer_sizes(jax.random.fold_in(keys[6], 71), 0)
    lars_skip = draw_lars_skip(jax.random.fold_in(keys[6], 71), 0)
    return dict(grads=grads, master=master, velocity=velocity, layer_offsets=layer_offsets, layer_sizes=layer_sizes, lars_skip=lars_skip)


def reference(grads, master, velocity, layer_offsets, layer_sizes, lars_skip):
    grad = lax.optimization_barrier(jnp.sum(grads.astype(jnp.float32), axis=(0, 1))) / (N_REPLICA * N_SPATIAL)
    position = jnp.arange(PARAMS, dtype=jnp.int32)
    inside = (position[None, :] >= layer_offsets[:, None]) & (position[None, :] < (layer_offsets + layer_sizes)[:, None])
    onehot = inside.astype(jnp.float32)
    wsq = jnp.dot(onehot, master * master, precision=lax.Precision.HIGHEST)
    gsq = jnp.dot(onehot, grad * grad, precision=lax.Precision.HIGHEST)
    wnorm = jnp.sqrt(wsq)
    gnorm = jnp.sqrt(gsq)
    skipped = lars_skip.astype(jnp.float32)
    ratio = 0.02 * wnorm / (gnorm + 0.001 * wnorm + 1e-06)
    trust = skipped + (1.0 - skipped) * ratio
    decay = (1.0 - skipped) * 0.001
    trust_pos = jnp.dot(trust, onehot, precision=lax.Precision.HIGHEST)
    decay_pos = jnp.dot(decay, onehot, precision=lax.Precision.HIGHEST)
    new_velocity = 0.9 * velocity + 8.0 * trust_pos * (grad + decay_pos * master)
    new_master = master - new_velocity
    return (new_master.astype(jnp.bfloat16), new_master, new_velocity)
```

```python
import jax
import jax.numpy as jnp
from jax import lax
from jax.experimental import pallas as pl
from jax.experimental.pallas import tpu as pltpu
from jax.sharding import Mesh
from jax.sharding import PartitionSpec as P

AXES = ("z", "x", "c", "y")
NZ, NX, NC, NY = 8, 4, 2, 8
NQ = NX * NC
LANES = 128
SHARD = 1666
BLOCK = NY * SHARD
ROWS = 6664
Z_ROWS = ROWS // NZ
Q_ROWS = 104
Y_ROWS = 13
SLOT = 16
TALL = 112
LAYERS = 6
f32 = jnp.float32
bf16 = jnp.bfloat16
VMEM = pl.BlockSpec(memory_space=pltpu.VMEM)
SMEM = pl.BlockSpec(memory_space=pltpu.SMEM)
PARAMS = pltpu.CompilerParams(vmem_limit_bytes=40 * 1024 * 1024)


def call(kernel, out_shape, ins, scratch=()):
    many = isinstance(out_shape, tuple)
    return pl.pallas_call(
        kernel,
        out_shape=out_shape,
        in_specs=list(ins),
        out_specs=(VMEM,) * len(out_shape) if many else VMEM,
        scratch_shapes=list(scratch),
        compiler_params=PARAMS,
    )


def row_of(z, q):
    return z * Z_ROWS + q * Q_ROWS


def pack_kernel(x_ref, o_ref):
    for z in range(NZ):
        for q in range(NQ):
            base = row_of(z, q)
            o_ref[q, z, :Q_ROWS, :] = x_ref[base : base + Q_ROWS, :].astype(bf16)
            last = x_ref[base + Q_ROWS : base + Q_ROWS + 1, :]
            o_ref[q, z, Q_ROWS:, :] = jnp.broadcast_to(last, (TALL - Q_ROWS, LANES)).astype(bf16)


def positions():
    z = lax.axis_index("z")
    q = lax.axis_index("x") * NC + lax.axis_index("c")
    row = lax.broadcasted_iota(jnp.int32, (TALL, LANES), 0)
    lane = lax.broadcasted_iota(jnp.int32, (TALL, LANES), 1)
    local = row * LANES + lane - 2 * NY * q
    valid = (local >= 0) & (local < BLOCK)
    return local + (z * NQ + q) * BLOCK, valid


def in_layer(tab_ref, l, pos):
    start = tab_ref[l]
    return (pos >= start) & (pos < start + tab_ref[LAYERS + l])


def norms_kernel(tab_ref, r_ref, n_ref, g_ref, m_ref, v_ref):
    g = r_ref[0, :TALL, :]
    for y in range(1, NY):
        g = g + r_ref[y, :TALL, :]
    g = g * (1.0 / 512.0)
    g_ref[...] = g
    m_ref[...] = jnp.zeros_like(m_ref)
    v_ref[...] = jnp.zeros_like(v_ref)
    for y in range(NY):
        rows = slice(y * Y_ROWS, y * Y_ROWS + Y_ROWS + 1)
        m_ref[rows, :] += r_ref[y, TALL : TALL + Y_ROWS + 1, :]
        v_ref[rows, :] += r_ref[y, TALL + SLOT : TALL + SLOT + Y_ROWS + 1, :]
    m = m_ref[...]
    pos, valid = positions()
    gg = jnp.where(valid, g * g, 0.0)
    mm = jnp.where(valid, m * m, 0.0)
    lane = lax.broadcasted_iota(jnp.int32, (1, LANES), 1)
    total = jnp.zeros((1, LANES), f32)
    for l in range(LAYERS):
        mask = in_layer(tab_ref, l, pos)
        for at, square in ((l, mm), (8 + l, gg)):
            rows = jnp.sum(jnp.where(mask, square, 0.0), axis=0, keepdims=True)
            total = total + jnp.where(lane == at, jnp.sum(rows, axis=1, keepdims=True), 0.0)
    n_ref[...] = jnp.broadcast_to(total[None], n_ref.shape)


def update_kernel(tab_ref, n_ref, g_ref, m_ref, v_ref, w_ref, om_ref, ov_ref, nm, nv, turn):
    norms = jnp.sum(n_ref[...], axis=0)
    lane1 = lax.broadcasted_iota(jnp.int32, (1, LANES), 1)
    pos, valid = positions()
    trust_pos = jnp.zeros((TALL, LANES), f32)
    decay_pos = jnp.zeros((TALL, LANES), f32)
    for l in range(LAYERS):
        wsq = jnp.sum(jnp.where(lane1 == l, norms, 0.0), axis=1, keepdims=True)
        gsq = jnp.sum(jnp.where(lane1 == 8 + l, norms, 0.0), axis=1, keepdims=True)
        wnorm, gnorm = jnp.sqrt(wsq), jnp.sqrt(gsq)
        skipped = tab_ref[2 * LAYERS + l].astype(f32)
        ratio = 0.02 * wnorm / (gnorm + 0.001 * wnorm + 1e-06)
        trust = skipped + (1.0 - skipped) * ratio
        mask = in_layer(tab_ref, l, pos)
        trust_pos = jnp.where(mask, trust, trust_pos)
        decay_pos = jnp.where(mask, (1.0 - skipped) * 0.001, decay_pos)
    m = m_ref[...]
    new_v = 0.9 * v_ref[...] + 8.0 * trust_pos * (g_ref[...] + decay_pos * m)
    new_m = m - new_v
    nm[...] = new_m
    nv[...] = new_v
    w = jnp.where(valid, new_m, 0.0).astype(bf16)
    for z in range(NZ):
        w_ref[z] = w
    q = lax.axis_index("x") * NC + lax.axis_index("c")
    y = lax.axis_index("y")
    shift = 2 * (NY * q + y)
    lane = lax.broadcasted_iota(jnp.int32, (SLOT, LANES), 1)
    for src, out in ((nm, om_ref), (nv, ov_ref)):
        own = src[:SLOT, :]
        for k in range(1, NY):
            own = jnp.where(y == k, src[k * Y_ROWS : k * Y_ROWS + SLOT, :], own)
        turned = pltpu.roll(own, lax.rem(LANES - shift, LANES), 1)
        turn[:SLOT, :] = turned
        turn[SLOT:, :] = jnp.zeros((8, LANES), f32)
        out[...] = jnp.where(lane < LANES - shift, turned, turn[1 : SLOT + 1, :])


def lay_out_kernel(a_ref, b_ref, o_ref, rows):
    c = lax.axis_index("c")
    for z in range(NZ):
        carry = None
        for q in range(NQ):
            x, cc = q // NC, q % NC
            mine, other = a_ref[x, z], b_ref[x, z]
            block = jnp.where(c == cc, mine.astype(f32), other.astype(f32))
            base = row_of(z, q)
            rows[base : base + Q_ROWS, :] = block[:Q_ROWS, :]
            if carry is not None:
                rows[base : base + 1, :] += carry
            carry = block[Q_ROWS : Q_ROWS + 1, :]
        rows[row_of(z, NQ) : row_of(z, NQ) + 1, :] = carry

    def narrow(k, _):
        at = pl.ds(pl.multiple_of(k * 136, 8), 136)
        o_ref[at, :] = rows[at, :].astype(bf16)
        return _

    lax.fori_loop(0, ROWS // 136, narrow, 0)


def sent(x, axes):
    return lax.all_to_all(x, axes, 0, 0, tiled=True)


def shards(grads, master, velocity, layer_offsets, layer_sizes, lars_skip):
    q = lax.axis_index("x") * NC + lax.axis_index("c")
    y = lax.axis_index("y")
    shift = 2 * (NY * q + y)
    tab = jnp.concatenate([layer_offsets, layer_sizes, lars_skip])

    def placed(a):
        flat = lax.dynamic_update_slice(jnp.zeros((SLOT * LANES,), f32), a, (shift,))
        return flat.reshape(SLOT, LANES)

    wide = grads.astype(f32).reshape(ROWS, LANES)
    packed = call(pack_kernel, jax.ShapeDtypeStruct((NQ, NZ, TALL, LANES), bf16), [VMEM])(wide)
    received = sent(packed, ("x", "c"))
    over_q = jnp.sum(received.astype(f32), axis=0)
    over_z = jnp.sum(sent(over_q, "z"), axis=0)
    mine = jnp.concatenate([over_z, placed(master), placed(velocity)])
    shared = sent(jnp.broadcast_to(mine, (NY, *mine.shape)), "y")
    tall = jax.ShapeDtypeStruct((TALL, LANES), f32)
    norms, g, m, v = call(
        norms_kernel,
        (jax.ShapeDtypeStruct((NZ * NQ, 1, LANES), f32), tall, tall, tall),
        [SMEM, VMEM],
    )(tab, shared)
    norms = sent(norms, ("z", "x", "c"))
    slot = jax.ShapeDtypeStruct((SLOT, LANES), f32)
    w, new_master, new_velocity = call(
        update_kernel,
        (jax.ShapeDtypeStruct((NZ, TALL, LANES), bf16), slot, slot),
        [SMEM, VMEM, VMEM, VMEM, VMEM],
        [
            pltpu.VMEM((TALL, LANES), f32),
            pltpu.VMEM((TALL, LANES), f32),
            pltpu.VMEM((SLOT + 8, LANES), f32),
        ],
    )(tab, norms, g, m, v)
    w = sent(w, "z")
    w = lax.all_gather(w.reshape(NZ * TALL, LANES), "x").reshape(NX, NZ, TALL, LANES)
    other = lax.ppermute(w, "c", [(0, 1), (1, 0)])
    weights = call(
        lay_out_kernel,
        jax.ShapeDtypeStruct((ROWS, LANES), bf16),
        [VMEM, VMEM],
        [pltpu.VMEM((ROWS, LANES), f32)],
    )(w, other)
    return (
        weights.reshape(ROWS * LANES),
        new_master.reshape(SLOT * LANES)[:SHARD],
        new_velocity.reshape(SLOT * LANES)[:SHARD],
    )


def solution(mesh):
    finer = Mesh(mesh.devices.reshape(NZ, NX, NC, NY), AXES)
    owned = P(AXES)
    in_specs = (P(("z", "x", "c"), "y", None), owned, owned, P(), P(), P())
    return jax.shard_map(
        shards, mesh=finer, in_specs=in_specs, out_specs=(P(), owned, owned), check_vma=False
    )
```

```python
import jax
import jax.numpy as jnp
from jax import lax
from jax.experimental import pallas as pl
from jax.experimental.pallas import tpu as pltpu
from jax.sharding import Mesh
from jax.sharding import PartitionSpec as P

AXES = ("z", "x", "c", "y")
NZ, NX, NC, NY = 8, 4, 2, 8
NQ = NX * NC
LANES = 128
SHARD = 1666
ROWS = 6664
Z_ROWS = ROWS // NZ
Q_ROWS = 104
Y_ROWS = 13
SLOT = 16
NORM_ROW = 14
TALL = 105
BLOCK_ROWS = NZ * TALL
LAYERS = 6
f32 = jnp.float32
bf16 = jnp.bfloat16
VMEM = pl.BlockSpec(memory_space=pltpu.VMEM)
SMEM = pl.BlockSpec(memory_space=pltpu.SMEM)
PARAMS = pltpu.CompilerParams(vmem_limit_bytes=40 * 1024 * 1024)


def shape(*dims, dtype=f32):
    return jax.ShapeDtypeStruct(dims, dtype)


def call(kernel, out_shape, ins, scratch=()):
    many = isinstance(out_shape, tuple)
    return pl.pallas_call(
        kernel,
        out_shape=out_shape,
        in_specs=list(ins),
        out_specs=(VMEM,) * len(out_shape) if many else VMEM,
        scratch_shapes=[pltpu.VMEM(s, f32) for s in scratch],
        compiler_params=PARAMS,
    )


def row_of(z, q):
    return z * Z_ROWS + q * Q_ROWS


def q_index():
    return lax.axis_index("x") * NC + lax.axis_index("c")


def pack_kernel(x_ref, o_ref, rows):
    for q in range(NQ):
        for z in range(NZ):
            base = row_of(z, q)
            rows[z * TALL : (z + 1) * TALL, :] = x_ref[base : base + TALL, :]
        o_ref[q] = rows[...].astype(bf16)


def spread_kernel(r_ref, o_ref, rows):
    total = r_ref[0].astype(f32)
    for q in range(1, NQ):
        total = total + r_ref[q].astype(f32)
    rows[...] = total
    for z in range(NZ):
        for y in range(NY):
            base = z * TALL + y * Y_ROWS
            o_ref[z * NY + y, :NORM_ROW, :] = rows[base : base + NORM_ROW, :]
            o_ref[z * NY + y, NORM_ROW:, :] = jnp.zeros((SLOT - NORM_ROW, LANES), f32)


def slot_positions():
    q, y = q_index(), lax.axis_index("y")
    owner = (lax.axis_index("z") * NQ + q) * NY + y
    row = lax.broadcasted_iota(jnp.int32, (SLOT, LANES), 0)
    lane = lax.broadcasted_iota(jnp.int32, (SLOT, LANES), 1)
    local = row * LANES + lane - 2 * (NY * q + y)
    return local + owner * SHARD, (local >= 0) & (local < SHARD)


def in_layer(tab_ref, l, pos):
    start = tab_ref[l]
    return (pos >= start) & (pos < start + tab_ref[LAYERS + l])


def skipped(tab_ref, l):
    return tab_ref[2 * LAYERS + l].astype(f32)


def owner_kernel(tab_ref, r_ref, m_ref, v_ref, o_ref, h_ref):
    g = r_ref[0]
    for k in range(1, NZ * NY):
        g = g + r_ref[k]
    pos, valid = slot_positions()
    g = jnp.where(valid, g * (1.0 / 512.0), 0.0)
    m = m_ref[...]
    lane = lax.broadcasted_iota(jnp.int32, (1, LANES), 1)
    total = jnp.zeros((1, LANES), f32)
    decay = jnp.zeros((SLOT, LANES), f32)
    for l in range(LAYERS):
        mask = in_layer(tab_ref, l, pos)
        decay = jnp.where(mask, (1.0 - skipped(tab_ref, l)) * 0.001, decay)
        for at, square in ((l, m * m), (8 + l, g * g)):
            rows = jnp.sum(jnp.where(mask, square, 0.0), axis=0, keepdims=True)
            total = total + jnp.where(lane == at, jnp.sum(rows, axis=1, keepdims=True), 0.0)
    h = g + decay * m
    h_ref[...] = h
    row = lax.broadcasted_iota(jnp.int32, (SLOT, LANES), 0)
    out = jnp.where(row == NORM_ROW, total, h)
    a = m - 0.9 * v_ref[...]
    for k in range(NZ * NY):
        o_ref[k, :SLOT, :] = out
        o_ref[k, SLOT:, :] = a


def group_kernel(s_ref, o_ref):
    total = s_ref[0, NORM_ROW : NORM_ROW + 1, :]
    for k in range(1, NZ * NY):
        total = total + s_ref[k, NORM_ROW : NORM_ROW + 1, :]
    o_ref[...] = jnp.broadcast_to(total[None], o_ref.shape)


def update_kernel(tab_ref, n_ref, s_ref, h_ref, m_ref, v_ref, w_ref, om_ref, ov_ref, hs, as_, turn):
    norms = jnp.sum(n_ref[...], axis=0)
    lane1 = lax.broadcasted_iota(jnp.int32, (1, LANES), 1)
    trusts = []
    for l in range(LAYERS):
        wsq = jnp.sum(jnp.where(lane1 == l, norms, 0.0), axis=1, keepdims=True)
        gsq = jnp.sum(jnp.where(lane1 == 8 + l, norms, 0.0), axis=1, keepdims=True)
        wnorm, gnorm = jnp.sqrt(wsq), jnp.sqrt(gsq)
        skip = skipped(tab_ref, l)
        ratio = 0.02 * wnorm / (gnorm + 0.001 * wnorm + 1e-06)
        trusts.append(skip + (1.0 - skip) * ratio)

    def trust_at(pos):
        trust = jnp.zeros(pos.shape, f32)
        for l in range(LAYERS):
            trust = jnp.where(in_layer(tab_ref, l, pos), trusts[l], trust)
        return trust

    for at, block in ((0, hs), (SLOT, as_)):
        for z in range(NZ):
            carry = None
            for y in range(NY):
                base = z * TALL + y * Y_ROWS
                block[base : base + Y_ROWS + 1, :] = s_ref[z * NY + y, at : at + Y_ROWS + 1, :]
                if carry is not None:
                    block[base : base + 1, :] += carry
                carry = s_ref[z * NY + y, at + Y_ROWS : at + Y_ROWS + 1, :]
    q = q_index()
    row = lax.broadcasted_iota(jnp.int32, (BLOCK_ROWS, LANES), 0)
    lane = lax.broadcasted_iota(jnp.int32, (BLOCK_ROWS, LANES), 1)
    extra = jnp.zeros((BLOCK_ROWS, LANES), jnp.int32)
    for z in range(1, NZ):
        extra = jnp.where(row >= z * TALL, z * (Z_ROWS - TALL), extra)
    pos = (row + extra + q * Q_ROWS) * LANES + lane
    w_ref[...] = (as_[...] - 8.0 * trust_at(pos) * hs[...]).astype(bf16)

    y = lax.axis_index("y")
    shift = 2 * (NY * q + y)
    pos, _ = slot_positions()
    new_v = 0.9 * v_ref[...] + 8.0 * trust_at(pos) * h_ref[...]
    new_m = m_ref[...] - new_v
    lane = lax.broadcasted_iota(jnp.int32, (SLOT, LANES), 1)
    for own, out in ((new_m, om_ref), (new_v, ov_ref)):
        turned = pltpu.roll(own, lax.rem(LANES - shift, LANES), 1)
        turn[:SLOT, :] = turned
        turn[SLOT:, :] = jnp.zeros((8, LANES), f32)
        out[...] = jnp.where(lane < LANES - shift, turned, turn[1 : SLOT + 1, :])


def lay_out_kernel(a_ref, b_ref, o_ref, block, rows):
    c = lax.axis_index("c")
    for q in range(NQ):
        x, cc = q // NC, q % NC
        block[...] = jnp.where(c == cc, a_ref[x].astype(f32), b_ref[x].astype(f32))
        for z in range(NZ):
            base = row_of(z, q)
            if q == 0:
                rows[base : base + TALL, :] = block[z * TALL : (z + 1) * TALL, :]
            else:
                rows[base : base + 1, :] += block[z * TALL : z * TALL + 1, :]
                rows[base + 1 : base + TALL, :] = block[z * TALL + 1 : (z + 1) * TALL, :]

    def narrow(k, _):
        at = pl.ds(pl.multiple_of(k * 136, 8), 136)
        o_ref[at, :] = rows[at, :].astype(bf16)
        return _

    lax.fori_loop(0, ROWS // 136, narrow, 0)


def sent(x, axes):
    return lax.all_to_all(x, axes, 0, 0, tiled=True)


def shards(grads, master, velocity, layer_offsets, layer_sizes, lars_skip):
    shift = 2 * (NY * q_index() + lax.axis_index("y"))
    tab = jnp.concatenate([layer_offsets, layer_sizes, lars_skip])

    def placed(a):
        flat = lax.dynamic_update_slice(jnp.zeros((SLOT * LANES,), f32), a, (shift,))
        return flat.reshape(SLOT, LANES)

    m, v, grads, tab = lax.optimization_barrier((placed(master), placed(velocity), grads, tab))
    wide = grads.astype(f32).reshape(ROWS, LANES)
    tall = (BLOCK_ROWS, LANES)
    packed = call(pack_kernel, shape(NQ, *tall, dtype=bf16), [VMEM], [tall])(wide)
    received = sent(packed, ("x", "c"))
    slots = shape(NZ * NY, SLOT, LANES)
    slot = shape(SLOT, LANES)
    spread = call(spread_kernel, slots, [VMEM], [tall])(received)
    reduced = sent(spread, ("z", "y"))
    pairs = shape(NZ * NY, 2 * SLOT, LANES)
    shared, h = call(owner_kernel, (pairs, slot), [SMEM] + [VMEM] * 3)(tab, reduced, m, v)
    shared = sent(shared, ("z", "y"))
    norms = call(group_kernel, shape(NQ, 1, LANES), [VMEM])(shared)
    norms = sent(norms, ("x", "c"))
    w, new_master, new_velocity = call(
        update_kernel,
        (shape(*tall, dtype=bf16), slot, slot),
        [SMEM] + [VMEM] * 5,
        [tall, tall, (SLOT + 8, LANES)],
    )(tab, norms, shared, h, m, v)
    w = lax.all_gather(w, "x")
    other = lax.ppermute(w, "c", [(0, 1), (1, 0)])
    weights = call(
        lay_out_kernel, shape(ROWS, LANES, dtype=bf16), [VMEM, VMEM], [tall, (ROWS, LANES)]
    )(w, other)
    return (
        weights.reshape(ROWS * LANES),
        new_master.reshape(SLOT * LANES)[:SHARD],
        new_velocity.reshape(SLOT * LANES)[:SHARD],
    )


def solution(mesh):
    finer = Mesh(mesh.devices.reshape(NZ, NX, NC, NY), AXES)
    owned = P(AXES)
    in_specs = (P(("z", "x", "c"), "y", None), owned, owned, P(), P(), P())

    return jax.shard_map(
        shards, mesh=finer, in_specs=in_specs, out_specs=(P(), owned, owned), check_vma=False
    )
```

```python
import jax
import jax.numpy as jnp
from jax import lax
from jax.experimental import pallas as pl
from jax.experimental.pallas import tpu as pltpu
from jax.sharding import Mesh
from jax.sharding import PartitionSpec as P

AXES = ("z", "x", "c", "y")
NZ, NX, NC, NY = 8, 4, 2, 8
NQ = NX * NC
LANES = 128
SHARD = 1666
ROWS = 6664
Z_ROWS = ROWS // NZ
Q_ROWS = 104
Y_ROWS = 13
SLOT = 16
NORM_ROW = 14
TOUCHED = 105
BLOCK_ROWS = NZ * TOUCHED
TALL = 112
LAYERS = 6
f32 = jnp.float32
bf16 = jnp.bfloat16
VMEM = pl.BlockSpec(memory_space=pltpu.VMEM)
SMEM = pl.BlockSpec(memory_space=pltpu.SMEM)
PARAMS = pltpu.CompilerParams(vmem_limit_bytes=40 * 1024 * 1024)


def shape(*dims, dtype=f32):
    return jax.ShapeDtypeStruct(dims, dtype)


def call(kernel, out_shape, ins, scratch=()):
    many = isinstance(out_shape, tuple)
    return pl.pallas_call(
        kernel,
        out_shape=out_shape,
        in_specs=list(ins),
        out_specs=(VMEM,) * len(out_shape) if many else VMEM,
        scratch_shapes=[pltpu.VMEM(s, f32) for s in scratch],
        compiler_params=PARAMS,
    )


def row_of(z, q):
    return z * Z_ROWS + q * Q_ROWS


def q_index():
    return lax.axis_index("x") * NC + lax.axis_index("c")


def pack_kernel(x_ref, o_ref, rows):
    for q in range(NQ):
        for z in range(NZ):
            base = row_of(z, q)
            rows[z * TOUCHED : (z + 1) * TOUCHED, :] = x_ref[base : base + TOUCHED, :]
        o_ref[q] = rows[...].astype(bf16)


def spread_kernel(r_ref, o_ref, rows):
    total = r_ref[0].astype(f32)
    for q in range(1, NQ):
        total = total + r_ref[q].astype(f32)
    rows[...] = total
    for z in range(NZ):
        for y in range(NY):
            base = z * TOUCHED + y * Y_ROWS
            o_ref[z * NY + y, :NORM_ROW, :] = rows[base : base + NORM_ROW, :]
            o_ref[z * NY + y, NORM_ROW:, :] = jnp.zeros((SLOT - NORM_ROW, LANES), f32)


def slot_positions():
    q, y = q_index(), lax.axis_index("y")
    owner = (lax.axis_index("z") * NQ + q) * NY + y
    row = lax.broadcasted_iota(jnp.int32, (SLOT, LANES), 0)
    lane = lax.broadcasted_iota(jnp.int32, (SLOT, LANES), 1)
    local = row * LANES + lane - 2 * (NY * q + y)
    return local + owner * SHARD, (local >= 0) & (local < SHARD)


def in_layer(tab_ref, l, pos):
    start = tab_ref[l]
    return (pos >= start) & (pos < start + tab_ref[LAYERS + l])


def skipped(tab_ref, l):
    return tab_ref[2 * LAYERS + l].astype(f32)


def owner_kernel(tab_ref, r_ref, m_ref, v_ref, o_ref, h_ref):
    g = r_ref[0]
    for k in range(1, NZ * NY):
        g = g + r_ref[k]
    pos, valid = slot_positions()
    g = jnp.where(valid, g * (1.0 / 512.0), 0.0)
    m = m_ref[...]
    lane = lax.broadcasted_iota(jnp.int32, (1, LANES), 1)
    total = jnp.zeros((1, LANES), f32)
    decay = jnp.zeros((SLOT, LANES), f32)
    for l in range(LAYERS):
        mask = in_layer(tab_ref, l, pos)
        decay = jnp.where(mask, (1.0 - skipped(tab_ref, l)) * 0.001, decay)
        for at, square in ((l, m * m), (8 + l, g * g)):
            rows = jnp.sum(jnp.where(mask, square, 0.0), axis=0, keepdims=True)
            total = total + jnp.where(lane == at, jnp.sum(rows, axis=1, keepdims=True), 0.0)
    h = g + decay * m
    h_ref[...] = h
    row = lax.broadcasted_iota(jnp.int32, (SLOT, LANES), 0)
    out = jnp.where(row == NORM_ROW, total, h)
    a = m - 0.9 * v_ref[...]
    for k in range(NY):
        o_ref[k, :SLOT, :] = out
        o_ref[k, SLOT:, :] = a


def group_kernel(s_ref, n_ref, hs_ref, as_ref):
    total = s_ref[0, NORM_ROW : NORM_ROW + 1, :]
    for y in range(1, NY):
        total = total + s_ref[y, NORM_ROW : NORM_ROW + 1, :]
    n_ref[...] = jnp.broadcast_to(total[None], n_ref.shape)
    for at, block in ((0, hs_ref), (SLOT, as_ref)):
        carry = None
        block[NY * Y_ROWS :, :] = jnp.zeros((TALL - NY * Y_ROWS, LANES), f32)
        for y in range(NY):
            base = y * Y_ROWS
            block[base : base + Y_ROWS + 1, :] = s_ref[y, at : at + Y_ROWS + 1, :]
            if carry is not None:
                block[base : base + 1, :] += carry
            carry = s_ref[y, at + Y_ROWS : at + Y_ROWS + 1, :]


def update_kernel(tab_ref, n_ref, hs_ref, as_ref, h_ref, m_ref, v_ref, w_ref, om_ref, ov_ref, turn):
    norms = jnp.sum(n_ref[...], axis=0)
    lane1 = lax.broadcasted_iota(jnp.int32, (1, LANES), 1)
    trusts = []
    for l in range(LAYERS):
        wsq = jnp.sum(jnp.where(lane1 == l, norms, 0.0), axis=1, keepdims=True)
        gsq = jnp.sum(jnp.where(lane1 == 8 + l, norms, 0.0), axis=1, keepdims=True)
        wnorm, gnorm = jnp.sqrt(wsq), jnp.sqrt(gsq)
        skip = skipped(tab_ref, l)
        ratio = 0.02 * wnorm / (gnorm + 0.001 * wnorm + 1e-06)
        trusts.append(skip + (1.0 - skip) * ratio)

    def trust_at(pos):
        trust = jnp.zeros(pos.shape, f32)
        for l in range(LAYERS):
            trust = jnp.where(in_layer(tab_ref, l, pos), trusts[l], trust)
        return trust

    q = q_index()
    row = lax.broadcasted_iota(jnp.int32, (TALL, LANES), 0)
    lane = lax.broadcasted_iota(jnp.int32, (TALL, LANES), 1)
    pos = (row + lax.axis_index("z") * Z_ROWS + q * Q_ROWS) * LANES + lane
    w = (as_ref[...] - 8.0 * trust_at(pos) * hs_ref[...]).astype(bf16)
    for z in range(NZ):
        w_ref[z] = w

    y = lax.axis_index("y")
    shift = 2 * (NY * q + y)
    pos, _ = slot_positions()
    new_v = 0.9 * v_ref[...] + 8.0 * trust_at(pos) * h_ref[...]
    new_m = m_ref[...] - new_v
    lane = lax.broadcasted_iota(jnp.int32, (SLOT, LANES), 1)
    for own, out in ((new_m, om_ref), (new_v, ov_ref)):
        turned = pltpu.roll(own, lax.rem(LANES - shift, LANES), 1)
        turn[:SLOT, :] = turned
        turn[SLOT:, :] = jnp.zeros((8, LANES), f32)
        out[...] = jnp.where(lane < LANES - shift, turned, turn[1 : SLOT + 1, :])


def lay_out_kernel(a_ref, b_ref, o_ref, rows):
    c = lax.axis_index("c")
    for z in range(NZ):
        carry = None
        for q in range(NQ):
            x, cc = q // NC, q % NC
            block = jnp.where(c == cc, a_ref[x, z].astype(f32), b_ref[x, z].astype(f32))
            base = row_of(z, q)
            rows[base : base + Q_ROWS, :] = block[:Q_ROWS, :]
            if carry is not None:
                rows[base : base + 1, :] += carry
            carry = block[Q_ROWS : Q_ROWS + 1, :]
        rows[row_of(z, NQ) : row_of(z, NQ) + 1, :] = carry

    def narrow(k, _):
        at = pl.ds(pl.multiple_of(k * 136, 8), 136)
        o_ref[at, :] = rows[at, :].astype(bf16)
        return _

    lax.fori_loop(0, ROWS // 136, narrow, 0)


def sent(x, axes):
    return lax.all_to_all(x, axes, 0, 0, tiled=True)


def shards(grads, master, velocity, layer_offsets, layer_sizes, lars_skip):
    shift = 2 * (NY * q_index() + lax.axis_index("y"))
    tab = jnp.concatenate([layer_offsets, layer_sizes, lars_skip])

    def placed(a):
        flat = lax.dynamic_update_slice(jnp.zeros((SLOT * LANES,), f32), a, (shift,))
        return flat.reshape(SLOT, LANES)

    m, v = placed(master), placed(velocity)
    wide = grads.astype(f32).reshape(ROWS, LANES)
    strip = (BLOCK_ROWS, LANES)
    packed = call(pack_kernel, shape(NQ, *strip, dtype=bf16), [VMEM], [strip])(wide)
    received = sent(packed, ("x", "c"))
    slots = shape(NZ * NY, SLOT, LANES)
    slot = shape(SLOT, LANES)
    spread = call(spread_kernel, slots, [VMEM], [strip])(received)
    reduced = sent(spread, ("z", "y"))
    pairs = shape(NY, 2 * SLOT, LANES)
    shared, h = call(owner_kernel, (pairs, slot), [SMEM] + [VMEM] * 3)(tab, reduced, m, v)
    tall = shape(TALL, LANES)
    norms, hs, as_ = call(group_kernel, (shape(NZ * NQ, 1, LANES), tall, tall), [VMEM])(
        sent(shared, "y")
    )
    w, new_master, new_velocity = call(
        update_kernel,
        (shape(NZ, TALL, LANES, dtype=bf16), slot, slot),
        [SMEM] + [VMEM] * 6,
        [(SLOT + 8, LANES)],
    )(tab, sent(norms, ("z", "x", "c")), hs, as_, h, m, v)
    w = sent(w, "z").reshape(NZ * TALL, LANES)
    w = lax.all_gather(w, "x").reshape(NX, NZ, TALL, LANES)
    other = lax.ppermute(w, "c", [(0, 1), (1, 0)])
    weights = call(
        lay_out_kernel, shape(ROWS, LANES, dtype=bf16), [VMEM, VMEM], [(ROWS, LANES)]
    )(w, other)
    return (
        weights.reshape(ROWS * LANES),
        new_master.reshape(SLOT * LANES)[:SHARD],
        new_velocity.reshape(SLOT * LANES)[:SHARD],
    )


def solution(mesh):
    finer = Mesh(mesh.devices.reshape(NZ, NX, NC, NY), AXES)
    owned = P(AXES)
    in_specs = (P(("z", "x", "c"), "y", None), owned, owned, P(), P(), P())

    return jax.shard_map(
        shards, mesh=finer, in_specs=in_specs, out_specs=(P(), owned, owned), check_vma=False
    )
```

```python
import jax
import jax.numpy as jnp
from jax import lax
from jax.experimental import pallas as pl
from jax.experimental.pallas import tpu as pltpu
from jax.sharding import Mesh
from jax.sharding import PartitionSpec as P

AXES = ("zh", "zl", "x", "c", "yh", "yl")
NEAR = ("zl", "x", "c", "yl")
FAR = ("zh", "yh")
NX, NC, NL, NH = 4, 2, 2, 4
NY, NZ = NH * NL, NH * NL
NQ = NX * NC
N_NEAR, N_FAR = NL * NQ * NL, NH * NH
LANES = 128
SHARD = 1666
ROWS = 6664
Z_ROWS = ROWS // NZ
Q_ROWS = 104
Y_ROWS = 13
TOUCHED = 14
SLOT = 16
NEAR_ROWS = N_FAR * TOUCHED
LAYERS = 6
f32 = jnp.float32
bf16 = jnp.bfloat16
VMEM = pl.BlockSpec(memory_space=pltpu.VMEM)
SMEM = pl.BlockSpec(memory_space=pltpu.SMEM)
PARAMS = pltpu.CompilerParams(vmem_limit_bytes=40 * 1024 * 1024)


def shape(*dims, dtype=f32):
    return jax.ShapeDtypeStruct(dims, dtype)


def call(kernel, out_shape, ins, scratch=()):
    many = isinstance(out_shape, tuple)
    return pl.pallas_call(
        kernel,
        out_shape=out_shape,
        in_specs=list(ins),
        out_specs=(VMEM,) * len(out_shape) if many else VMEM,
        scratch_shapes=[pltpu.VMEM(s, f32) for s in scratch],
        compiler_params=PARAMS,
    )


def row_of(z, q, y):
    return z * Z_ROWS + q * Q_ROWS + y * Y_ROWS


def z_index():
    return lax.axis_index("zh") * NL + lax.axis_index("zl")


def q_index():
    return lax.axis_index("x") * NC + lax.axis_index("c")


def y_index():
    return lax.axis_index("yh") * NL + lax.axis_index("yl")


def far_slots():
    return [(k, k // NH, k % NH) for k in range(N_FAR)]


def pack_kernel(x_ref, o_ref, rows):
    for near in range(N_NEAR):
        zl, q, yl = near // (NQ * NL), near // NL % NQ, near % NL
        for k, zh, yh in far_slots():
            base = row_of(zh * NL + zl, q, yh * NL + yl)
            rows[k * TOUCHED : (k + 1) * TOUCHED, :] = x_ref[base : base + TOUCHED, :]
        o_ref[near] = rows[...].astype(bf16)


def spread_kernel(r_ref, o_ref, rows):
    total = r_ref[0].astype(f32)
    for k in range(1, N_NEAR):
        total = total + r_ref[k].astype(f32)
    rows[...] = total
    for k in range(N_FAR):
        o_ref[k, :TOUCHED, :] = rows[k * TOUCHED : (k + 1) * TOUCHED, :]
        o_ref[k, TOUCHED:, :] = jnp.zeros((SLOT - TOUCHED, LANES), f32)


def slot_positions():
    q, y = q_index(), y_index()
    owner = (z_index() * NQ + q) * NY + y
    row = lax.broadcasted_iota(jnp.int32, (SLOT, LANES), 0)
    lane = lax.broadcasted_iota(jnp.int32, (SLOT, LANES), 1)
    local = row * LANES + lane - 2 * (NY * q + y)
    return local + owner * SHARD, (local >= 0) & (local < SHARD)


def in_layer(tab_ref, l, pos):
    start = tab_ref[l]
    return (pos >= start) & (pos < start + tab_ref[LAYERS + l])


def skipped(tab_ref, l):
    return tab_ref[2 * LAYERS + l].astype(f32)


def owner_kernel(tab_ref, r_ref, m_ref, v_ref, o_ref, h_ref):
    g = r_ref[0]
    for k in range(1, N_FAR):
        g = g + r_ref[k]
    pos, valid = slot_positions()
    g = jnp.where(valid, g * (1.0 / 512.0), 0.0)
    m = m_ref[...]
    lane = lax.broadcasted_iota(jnp.int32, (1, LANES), 1)
    total = jnp.zeros((1, LANES), f32)
    decay = jnp.zeros((SLOT, LANES), f32)
    for l in range(LAYERS):
        mask = in_layer(tab_ref, l, pos)
        decay = jnp.where(mask, (1.0 - skipped(tab_ref, l)) * 0.001, decay)
        for at, square in ((l, m * m), (8 + l, g * g)):
            rows = jnp.sum(jnp.where(mask, square, 0.0), axis=0, keepdims=True)
            total = total + jnp.where(lane == at, jnp.sum(rows, axis=1, keepdims=True), 0.0)
    h = g + decay * m
    h_ref[...] = h
    row = lax.broadcasted_iota(jnp.int32, (SLOT, LANES), 0)
    out = jnp.where(row == TOUCHED, total, h)
    a = m - 0.9 * v_ref[...]
    for k in range(N_FAR):
        o_ref[k, :SLOT, :] = out
        o_ref[k, SLOT:, :] = a


def group_kernel(s_ref, n_ref):
    total = s_ref[0, TOUCHED : TOUCHED + 1, :]
    for k in range(1, N_FAR):
        total = total + s_ref[k, TOUCHED : TOUCHED + 1, :]
    n_ref[...] = jnp.broadcast_to(total[None], n_ref.shape)


def update_kernel(tab_ref, n_ref, s_ref, h_ref, m_ref, v_ref, w_ref, om_ref, ov_ref, rows, turn):
    norms = jnp.sum(n_ref[...], axis=0)
    lane1 = lax.broadcasted_iota(jnp.int32, (1, LANES), 1)
    trusts = []
    for l in range(LAYERS):
        wsq = jnp.sum(jnp.where(lane1 == l, norms, 0.0), axis=1, keepdims=True)
        gsq = jnp.sum(jnp.where(lane1 == 8 + l, norms, 0.0), axis=1, keepdims=True)
        wnorm, gnorm = jnp.sqrt(wsq), jnp.sqrt(gsq)
        skip = skipped(tab_ref, l)
        ratio = 0.02 * wnorm / (gnorm + 0.001 * wnorm + 1e-06)
        trusts.append(skip + (1.0 - skip) * ratio)

    def trust_at(pos):
        trust = jnp.zeros(pos.shape, f32)
        for l in range(LAYERS):
            trust = jnp.where(in_layer(tab_ref, l, pos), trusts[l], trust)
        return trust

    q = q_index()
    at = lax.broadcasted_iota(jnp.int32, (SLOT, LANES), 0) * LANES
    at = at + lax.broadcasted_iota(jnp.int32, (SLOT, LANES), 1)
    for k, zh, yh in far_slots():
        z, y = zh * NL + lax.axis_index("zl"), yh * NL + lax.axis_index("yl")
        pos = at + row_of(z, q, y) * LANES
        w = s_ref[k, SLOT:, :] - 8.0 * trust_at(pos) * s_ref[k, :SLOT, :]
        rows[k * TOUCHED : (k + 1) * TOUCHED, :] = w[:TOUCHED, :]
    w = rows[...].astype(bf16)
    for k in range(NL * NX * NL):
        w_ref[k] = w

    shift = 2 * (NY * q + y_index())
    pos, _ = slot_positions()
    new_v = 0.9 * v_ref[...] + 8.0 * trust_at(pos) * h_ref[...]
    new_m = m_ref[...] - new_v
    lane = lax.broadcasted_iota(jnp.int32, (SLOT, LANES), 1)
    for own, out in ((new_m, om_ref), (new_v, ov_ref)):
        turned = pltpu.roll(own, lax.rem(LANES - shift, LANES), 1)
        turn[:SLOT, :] = turned
        turn[SLOT:, :] = jnp.zeros((8, LANES), f32)
        out[...] = jnp.where(lane < LANES - shift, turned, turn[1 : SLOT + 1, :])


def lay_out_kernel(a_ref, b_ref, o_ref, block, tail, rows):
    c = lax.axis_index("c")
    for near in range(N_NEAR):
        zl, q, yl = near // (NQ * NL), near // NL % NQ, near % NL
        cc, peer = q % NC, (zl * NX + q // NC) * NL + yl
        block[...] = jnp.where(c == cc, a_ref[peer].astype(f32), b_ref[peer].astype(f32))
        for k, zh, yh in far_slots():
            z, y = zh * NL + zl, yh * NL + yl
            base, at = row_of(z, q, y), k * TOUCHED
            rows[base : base + Y_ROWS, :] = block[at : at + Y_ROWS, :]
            owner = (z * NQ + q) * NY + y
            tail[owner : owner + 1, :] = block[at + Y_ROWS : at + TOUCHED, :]
    for z in range(NZ):
        for k in range(NQ * NY):
            q, y = k // NY, k % NY
            base, owner = row_of(z, q, y), z * NQ * NY + k
            if k + 1 < NQ * NY:
                rows[base + Y_ROWS : base + TOUCHED, :] += tail[owner : owner + 1, :]
            else:
                rows[base + Y_ROWS : base + TOUCHED, :] = tail[owner : owner + 1, :]

    def narrow(k, _):
        at = pl.ds(pl.multiple_of(k * 136, 8), 136)
        o_ref[at, :] = rows[at, :].astype(bf16)
        return _

    lax.fori_loop(0, ROWS // 136, narrow, 0)


def sent(x, axes):
    return lax.all_to_all(x, axes, 0, 0, tiled=True)


def shards(grads, master, velocity, layer_offsets, layer_sizes, lars_skip):
    shift = 2 * (NY * q_index() + y_index())
    tab = jnp.concatenate([layer_offsets, layer_sizes, lars_skip])

    def placed(a):
        flat = lax.dynamic_update_slice(jnp.zeros((SLOT * LANES,), f32), a, (shift,))
        return flat.reshape(SLOT, LANES)

    m, v = placed(master), placed(velocity)
    wide = grads.astype(f32).reshape(ROWS, LANES)
    wide, m, v, tab = lax.optimization_barrier((wide, m, v, tab))
    near, far, slot = (NEAR_ROWS, LANES), (SLOT, LANES), shape(SLOT, LANES)
    packed = call(pack_kernel, shape(N_NEAR, *near, dtype=bf16), [VMEM], [near])(wide)
    spread = call(spread_kernel, shape(N_FAR, *far), [VMEM], [near])(sent(packed, NEAR))
    shared, h = call(
        owner_kernel, (shape(N_FAR, 2 * SLOT, LANES), slot), [SMEM] + [VMEM] * 3
    )(tab, sent(spread, FAR), m, v)
    shared = sent(shared, FAR)
    norms = call(group_kernel, shape(N_NEAR, 1, LANES), [VMEM])(shared)
    w, new_master, new_velocity = call(
        update_kernel,
        (shape(NL * NX * NL, *near, dtype=bf16), slot, slot),
        [SMEM] + [VMEM] * 5,
        [near, (SLOT + 8, LANES)],
    )(tab, sent(norms, NEAR), shared, h, m, v)
    w = sent(w, ("zl", "x", "yl"))
    other = lax.ppermute(w, "c", [(0, 1), (1, 0)])
    weights = call(
        lay_out_kernel,
        shape(ROWS, LANES, dtype=bf16),
        [VMEM, VMEM],
        [near, (N_NEAR * N_FAR, LANES), (ROWS, LANES)],
    )(w, other)
    return (
        weights.reshape(ROWS * LANES),
        new_master.reshape(SLOT * LANES)[:SHARD],
        new_velocity.reshape(SLOT * LANES)[:SHARD],
    )


def solution(mesh):
    finer = Mesh(mesh.devices.reshape(NH, NL, NX, NC, NH, NL), AXES)
    owned = P(AXES)
    in_specs = (P(("zh", "zl", "x", "c"), ("yh", "yl"), None), owned, owned, P(), P(), P())
    return jax.shard_map(
        shards, mesh=finer, in_specs=in_specs, out_specs=(P(), owned, owned), check_vma=False
    )
```

```python
import jax
import jax.numpy as jnp
from jax import lax
from jax.experimental import pallas as pl
from jax.experimental.pallas import tpu as pltpu
from jax.sharding import Mesh
from jax.sharding import PartitionSpec as P

AXES = ("zh", "zl", "x", "c", "yh", "yl")
NEAR = ("zl", "x", "c", "yl")
FAR = ("zh", "yh")
NX, NC, NL, NH = 4, 2, 2, 4
NY, NZ = NH * NL, NH * NL
NQ = NX * NC
N_NEAR, N_FAR = NL * NQ * NL, NH * NH
LANES = 128
SHARD = 1666
ROWS = 6664
Z_ROWS = ROWS // NZ
Q_ROWS = 104
Y_ROWS = 13
TOUCHED = 14
SLOT = 16
NEAR_ROWS = N_FAR * TOUCHED
LAYERS = 6
STEPS = 7
STEP_ROWS = ROWS // STEPS
CHUNK = 136
f32 = jnp.float32
bf16 = jnp.bfloat16
VMEM = pl.BlockSpec(memory_space=pltpu.VMEM)
SMEM = pl.BlockSpec(memory_space=pltpu.SMEM)
PARAMS = pltpu.CompilerParams(vmem_limit_bytes=40 * 1024 * 1024)


def shape(*dims, dtype=f32):
    return jax.ShapeDtypeStruct(dims, dtype)


def call(kernel, out_shape, ins, scratch=()):
    many = isinstance(out_shape, tuple)
    return pl.pallas_call(
        kernel,
        out_shape=out_shape,
        in_specs=list(ins),
        out_specs=(VMEM,) * len(out_shape) if many else VMEM,
        scratch_shapes=[pltpu.VMEM(s, f32) for s in scratch],
        compiler_params=PARAMS,
    )


def row_of(z, q, y):
    return z * Z_ROWS + q * Q_ROWS + y * Y_ROWS


def z_index():
    return lax.axis_index("zh") * NL + lax.axis_index("zl")


def q_index():
    return lax.axis_index("x") * NC + lax.axis_index("c")


def y_index():
    return lax.axis_index("yh") * NL + lax.axis_index("yl")


def far_slots():
    return [(k, k // NH, k % NH) for k in range(N_FAR)]


def pack_kernel(x_ref, o_ref, held, sems, wide, rows):
    copies = []
    for i in range(STEPS):
        at = pl.ds(i * STEP_ROWS, STEP_ROWS)
        copies.append(pltpu.make_async_copy(x_ref.at[at], held.at[at], sems.at[i]))
        copies[-1].start()
    for i in range(STEPS):
        copies[i].wait()

        def widen(k, _):
            at = i * STEP_ROWS + k * CHUNK
            for r in range(CHUNK):
                wide[pl.ds(at + r, 1), :] = held[at + r].astype(f32)
            return _

        lax.fori_loop(0, STEP_ROWS // CHUNK, widen, 0)
    for near in range(N_NEAR):
        zl, q, yl = near // (NQ * NL), near // NL % NQ, near % NL
        for k, zh, yh in far_slots():
            base = row_of(zh * NL + zl, q, yh * NL + yl)
            rows[k * TOUCHED : (k + 1) * TOUCHED, :] = wide[base : base + TOUCHED, :]
        o_ref[near] = rows[...].astype(bf16)


def packed(grads):
    return pl.pallas_call(
        pack_kernel,
        out_shape=shape(N_NEAR, NEAR_ROWS, LANES, dtype=bf16),
        in_specs=[pl.BlockSpec(memory_space=pl.ANY)],
        out_specs=VMEM,
        scratch_shapes=[
            pltpu.VMEM((ROWS, 1, LANES), bf16),
            pltpu.SemaphoreType.DMA((STEPS,)),
            pltpu.VMEM((ROWS, LANES), f32),
            pltpu.VMEM((NEAR_ROWS, LANES), f32),
        ],
        compiler_params=pltpu.CompilerParams(vmem_limit_bytes=51 * 1024 * 1024),
    )(grads.reshape(ROWS, 1, LANES))


def spread_kernel(r_ref, o_ref, rows):
    total = r_ref[0].astype(f32)
    for k in range(1, N_NEAR):
        total = total + r_ref[k].astype(f32)
    rows[...] = total
    for k in range(N_FAR):
        o_ref[k, :TOUCHED, :] = rows[k * TOUCHED : (k + 1) * TOUCHED, :]
        o_ref[k, TOUCHED:, :] = jnp.zeros((SLOT - TOUCHED, LANES), f32)


def slot_positions():
    q, y = q_index(), y_index()
    owner = (z_index() * NQ + q) * NY + y
    row = lax.broadcasted_iota(jnp.int32, (SLOT, LANES), 0)
    lane = lax.broadcasted_iota(jnp.int32, (SLOT, LANES), 1)
    local = row * LANES + lane - 2 * (NY * q + y)
    return local + owner * SHARD, (local >= 0) & (local < SHARD)


def in_layer(tab_ref, l, pos):
    start = tab_ref[l]
    return (pos >= start) & (pos < start + tab_ref[LAYERS + l])


def skipped(tab_ref, l):
    return tab_ref[2 * LAYERS + l].astype(f32)


def owner_kernel(tab_ref, r_ref, m_ref, v_ref, o_ref, h_ref):
    g = r_ref[0]
    for k in range(1, N_FAR):
        g = g + r_ref[k]
    pos, valid = slot_positions()
    g = jnp.where(valid, g * (1.0 / 512.0), 0.0)
    m = m_ref[...]
    lane = lax.broadcasted_iota(jnp.int32, (1, LANES), 1)
    total = jnp.zeros((1, LANES), f32)
    decay = jnp.zeros((SLOT, LANES), f32)
    for l in range(LAYERS):
        mask = in_layer(tab_ref, l, pos)
        decay = jnp.where(mask, (1.0 - skipped(tab_ref, l)) * 0.001, decay)
        for at, square in ((l, m * m), (8 + l, g * g)):
            rows = jnp.sum(jnp.where(mask, square, 0.0), axis=0, keepdims=True)
            total = total + jnp.where(lane == at, jnp.sum(rows, axis=1, keepdims=True), 0.0)
    h = g + decay * m
    h_ref[...] = h
    row = lax.broadcasted_iota(jnp.int32, (SLOT, LANES), 0)
    out = jnp.where(row == TOUCHED, total, h)
    a = m - 0.9 * v_ref[...]
    for k in range(N_FAR):
        o_ref[k, :SLOT, :] = out
        o_ref[k, SLOT:, :] = a


def group_kernel(s_ref, n_ref):
    total = s_ref[0, TOUCHED : TOUCHED + 1, :]
    for k in range(1, N_FAR):
        total = total + s_ref[k, TOUCHED : TOUCHED + 1, :]
    n_ref[...] = jnp.broadcast_to(total[None], n_ref.shape)


def trust_at(tab_ref, trust, pos):
    lane = lax.broadcasted_iota(jnp.int32, (1, LANES), 1)
    out = jnp.zeros(pos[0].shape, f32)
    outs = [out] * len(pos)
    for l in range(LAYERS):
        one = jnp.sum(jnp.where(lane == l, trust, 0.0), axis=1, keepdims=True)
        outs = [jnp.where(in_layer(tab_ref, l, p), one, o) for p, o in zip(pos, outs)]
    return outs


def update_kernel(tab_ref, n_ref, s_ref, w_ref, t_ref, rows):
    norms = jnp.sum(n_ref[...], axis=0)
    lane = lax.broadcasted_iota(jnp.int32, (1, LANES), 1)
    skip = jnp.zeros((1, LANES), f32)
    for l in range(LAYERS):
        skip = jnp.where(lane == l, skipped(tab_ref, l), skip)
    wnorm = jnp.sqrt(norms)
    gnorm = pltpu.roll(wnorm, LANES - 8, 1)
    ratio = 0.02 * wnorm / (gnorm + 0.001 * wnorm + 1e-06)
    trust = skip + (1.0 - skip) * ratio
    t_ref[...] = trust
    at = lax.broadcasted_iota(jnp.int32, (SLOT, LANES), 0) * LANES
    at = at + lax.broadcasted_iota(jnp.int32, (SLOT, LANES), 1)
    pos = [
        at + row_of(zh * NL + lax.axis_index("zl"), q_index(), yh * NL + lax.axis_index("yl")) * LANES
        for _, zh, yh in far_slots()
    ]
    for k, t in enumerate(trust_at(tab_ref, trust, pos)):
        w = s_ref[k, SLOT:, :] - 8.0 * t * s_ref[k, :SLOT, :]
        rows[k * TOUCHED : (k + 1) * TOUCHED, :] = w[:TOUCHED, :]
    w = rows[...].astype(bf16)
    for k in range(NL * NX * NL):
        w_ref[k] = w


def own_kernel(tab_ref, t_ref, h_ref, m_ref, v_ref, om_ref, ov_ref, turn):
    shift = 2 * (NY * q_index() + y_index())
    pos, _ = slot_positions()
    (trust,) = trust_at(tab_ref, t_ref[...], [pos])
    new_v = 0.9 * v_ref[...] + 8.0 * trust * h_ref[...]
    new_m = m_ref[...] - new_v
    lane = lax.broadcasted_iota(jnp.int32, (SLOT, LANES), 1)
    for own, out in ((new_m, om_ref), (new_v, ov_ref)):
        turned = pltpu.roll(own, lax.rem(LANES - shift, LANES), 1)
        turn[:SLOT, :] = turned
        turn[SLOT:, :] = jnp.zeros((8, LANES), f32)
        out[...] = jnp.where(lane < LANES - shift, turned, turn[1 : SLOT + 1, :])


def put_core(w_ref, c, block, rows, tail):
    for peer in range(NL * NX * NL):
        zl, x, yl = peer // (NX * NL), peer // NL % NX, peer % NL
        block[...] = w_ref[peer].astype(f32)
        for k, zh, yh in far_slots():
            z, y = zh * NL + zl, yh * NL + yl
            at, q = k * TOUCHED, x * NC
            owner = (z * NQ + q) * NY + y
            base = row_of(z, q, y) + c * Q_ROWS
            rows[pl.ds(base, Y_ROWS), :] = block[at : at + Y_ROWS, :]
            tail[pl.ds(owner + c * NY, 1), :] = block[at + Y_ROWS : at + TOUCHED, :]


def own_half_kernel(w_ref, rows, tail, block):
    put_core(w_ref, lax.axis_index("c"), block, rows, tail)


def lay_out_kernel(w_ref, rows, tail, o_ref, block):
    put_core(w_ref, 1 - lax.axis_index("c"), block, rows, tail)
    for z in range(NZ):
        for k in range(NQ * NY):
            base, owner = row_of(z, k // NY, k % NY), z * NQ * NY + k
            if k + 1 < NQ * NY:
                rows[base + Y_ROWS : base + TOUCHED, :] += tail[owner : owner + 1, :]
            else:
                rows[base + Y_ROWS : base + TOUCHED, :] = tail[owner : owner + 1, :]

    def narrow(k, _):
        at = pl.ds(pl.multiple_of(k * 136, 8), 136)
        o_ref[at, :] = rows[at, :].astype(bf16)
        return _

    lax.fori_loop(0, ROWS // 136, narrow, 0)


def sent(x, axes):
    return lax.all_to_all(x, axes, 0, 0, tiled=True)


def shards(grads, master, velocity, layer_offsets, layer_sizes, lars_skip):
    shift = 2 * (NY * q_index() + y_index())
    tab = jnp.concatenate([layer_offsets, layer_sizes, lars_skip])

    def placed(a):
        flat = lax.dynamic_update_slice(jnp.zeros((SLOT * LANES,), f32), a, (shift,))
        return flat.reshape(SLOT, LANES)

    m, v = placed(master), placed(velocity)
    near, far, slot = (NEAR_ROWS, LANES), (SLOT, LANES), shape(SLOT, LANES)
    sending, m, v, tab = lax.optimization_barrier((packed(grads), m, v, tab))
    spread = call(spread_kernel, shape(N_FAR, *far), [VMEM], [near])(sent(sending, NEAR))
    shared, h = call(
        owner_kernel, (shape(N_FAR, 2 * SLOT, LANES), slot), [SMEM] + [VMEM] * 3
    )(tab, sent(spread, FAR), m, v)
    shared = sent(shared, FAR)
    norms = call(group_kernel, shape(N_NEAR, 1, LANES), [VMEM])(shared)
    w, trust = call(
        update_kernel,
        (shape(NL * NX * NL, *near, dtype=bf16), shape(1, LANES)),
        [SMEM, VMEM, VMEM],
        [near],
    )(tab, sent(norms, NEAR), shared)
    w = sent(w, ("zl", "x", "yl"))
    other = lax.ppermute(w, "c", [(0, 1), (1, 0)])
    rows, tail = call(
        own_half_kernel, (shape(ROWS, LANES), shape(N_NEAR * N_FAR, LANES)), [VMEM], [near]
    )(w)
    new_master, new_velocity = call(
        own_kernel, (slot, slot), [SMEM] + [VMEM] * 4, [(SLOT + 8, LANES)]
    )(tab, trust, h, m, v)
    _, _, weights = pl.pallas_call(
        lambda w_ref, r_in, t_in, rows, tail, o_ref, block: lay_out_kernel(
            w_ref, rows, tail, o_ref, block
        ),
        out_shape=(
            shape(ROWS, LANES),
            shape(N_NEAR * N_FAR, LANES),
            shape(ROWS, LANES, dtype=bf16),
        ),
        in_specs=[VMEM] * 3,
        out_specs=(VMEM,) * 3,
        input_output_aliases={1: 0, 2: 1},
        scratch_shapes=[pltpu.VMEM(near, f32)],
        compiler_params=PARAMS,
    )(other, rows, tail)
    return (
        weights.reshape(ROWS * LANES),
        new_master.reshape(SLOT * LANES)[:SHARD],
        new_velocity.reshape(SLOT * LANES)[:SHARD],
    )


def solution(mesh):
    finer = Mesh(mesh.devices.reshape(NH, NL, NX, NC, NH, NL), AXES)
    owned = P(AXES)
    in_specs = (P(("zh", "zl", "x", "c"), ("yh", "yl"), None), owned, owned, P(), P(), P())
    return jax.shard_map(
        shards, mesh=finer, in_specs=in_specs, out_specs=(P(), owned, owned), check_vma=False
    )
```

```python
import jax
import jax.numpy as jnp
from jax import lax
from jax.experimental import pallas as pl
from jax.experimental.pallas import tpu as pltpu
from jax.sharding import Mesh
from jax.sharding import PartitionSpec as P

AXES = ("zh", "zl", "x", "c", "yh", "yl")
NEAR = ("zl", "x", "c", "yl")
FAR = ("zh", "yh")
NX, NC, NL, NH = 4, 2, 2, 4
NY, NZ = NH * NL, NH * NL
NQ = NX * NC
N_NEAR, N_FAR = NL * NQ * NL, NH * NH
LANES = 128
SHARD = 1666
ROWS = 6664
Z_ROWS = ROWS // NZ
Q_ROWS = 104
Y_ROWS = 13
TOUCHED = 14
SLOT = 16
NEAR_ROWS = N_FAR * TOUCHED
LAYERS = 6
STEPS = 7
STEP_ROWS = ROWS // STEPS
CHUNK = 136
f32 = jnp.float32
bf16 = jnp.bfloat16
VMEM = pl.BlockSpec(memory_space=pltpu.VMEM)
SMEM = pl.BlockSpec(memory_space=pltpu.SMEM)
PARAMS = pltpu.CompilerParams(vmem_limit_bytes=40 * 1024 * 1024)


def shape(*dims, dtype=f32):
    return jax.ShapeDtypeStruct(dims, dtype)


def call(kernel, out_shape, ins, scratch=()):
    many = isinstance(out_shape, tuple)
    return pl.pallas_call(
        kernel,
        out_shape=out_shape,
        in_specs=list(ins),
        out_specs=(VMEM,) * len(out_shape) if many else VMEM,
        scratch_shapes=[pltpu.VMEM(s, f32) for s in scratch],
        compiler_params=PARAMS,
    )


def row_of(z, q, y):
    return z * Z_ROWS + q * Q_ROWS + y * Y_ROWS


def z_index():
    return lax.axis_index("zh") * NL + lax.axis_index("zl")


def q_index():
    return lax.axis_index("x") * NC + lax.axis_index("c")


def y_index():
    return lax.axis_index("yh") * NL + lax.axis_index("yl")


def far_slots():
    return [(k, k // NH, k % NH) for k in range(N_FAR)]


def pack_kernel(x_ref, o_ref, held, sems, wide, rows):
    copies = []
    for i in range(STEPS):
        at = pl.ds(i * STEP_ROWS, STEP_ROWS)
        copies.append(pltpu.make_async_copy(x_ref.at[at], held.at[at], sems.at[i]))
        copies[-1].start()
    for i in range(STEPS):
        copies[i].wait()

        def widen(k, _):
            at = i * STEP_ROWS + k * CHUNK
            for r in range(CHUNK):
                wide[pl.ds(at + r, 1), :] = held[at + r].astype(f32)
            return _

        lax.fori_loop(0, STEP_ROWS // CHUNK, widen, 0)
    for near in range(N_NEAR):
        zl, q, yl = near // (NQ * NL), near // NL % NQ, near % NL
        for k, zh, yh in far_slots():
            base = row_of(zh * NL + zl, q, yh * NL + yl)
            rows[k * TOUCHED : (k + 1) * TOUCHED, :] = wide[base : base + TOUCHED, :]
        o_ref[near] = rows[...].astype(bf16)


def packed(grads):
    return pl.pallas_call(
        pack_kernel,
        out_shape=shape(N_NEAR, NEAR_ROWS, LANES, dtype=bf16),
        in_specs=[pl.BlockSpec(memory_space=pl.ANY)],
        out_specs=VMEM,
        scratch_shapes=[
            pltpu.VMEM((ROWS, 1, LANES), bf16),
            pltpu.SemaphoreType.DMA((STEPS,)),
            pltpu.VMEM((ROWS, LANES), f32),
            pltpu.VMEM((NEAR_ROWS, LANES), f32),
        ],
        compiler_params=pltpu.CompilerParams(vmem_limit_bytes=51 * 1024 * 1024),
    )(grads.reshape(ROWS, 1, LANES))


def spread_kernel(r_ref, o_ref, rows):
    total = r_ref[0].astype(f32)
    for k in range(1, N_NEAR):
        total = total + r_ref[k].astype(f32)
    rows[...] = total
    for k in range(N_FAR):
        o_ref[k, :TOUCHED, :] = rows[k * TOUCHED : (k + 1) * TOUCHED, :]
        o_ref[k, TOUCHED:, :] = jnp.zeros((SLOT - TOUCHED, LANES), f32)


def slot_positions():
    q, y = q_index(), y_index()
    owner = (z_index() * NQ + q) * NY + y
    row = lax.broadcasted_iota(jnp.int32, (SLOT, LANES), 0)
    lane = lax.broadcasted_iota(jnp.int32, (SLOT, LANES), 1)
    local = row * LANES + lane - 2 * (NY * q + y)
    return local + owner * SHARD, (local >= 0) & (local < SHARD)


def in_layer(tab_ref, l, pos):
    start = tab_ref[l]
    return (pos >= start) & (pos < start + tab_ref[LAYERS + l])


def skipped(tab_ref, l):
    return tab_ref[2 * LAYERS + l].astype(f32)


def placed(flat_ref, rows):
    whole = SHARD // LANES
    rows[...] = jnp.zeros((SLOT + 8, LANES), f32)
    for k in range(whole):
        rows[8 + k, :] = flat_ref[pl.ds(k * LANES, LANES)]
    rows[8 + whole, pl.ds(0, SHARD - whole * LANES)] = flat_ref[pl.ds(whole * LANES, SHARD - whole * LANES)]
    shift = 2 * (NY * q_index() + y_index())
    lane = lax.broadcasted_iota(jnp.int32, (SLOT, LANES), 1)
    here = pltpu.roll(rows[8:, :], shift, 1)
    above = pltpu.roll(rows[7 : SLOT + 7, :], shift, 1)
    return jnp.where(lane >= shift, here, above)


def owner_kernel(tab_ref, r_ref, mf_ref, vf_ref, o_ref, h_ref, m_ref, v_ref, rows):
    m_ref[...] = placed(mf_ref, rows)
    v_ref[...] = placed(vf_ref, rows)
    g = r_ref[0]
    for k in range(1, N_FAR):
        g = g + r_ref[k]
    pos, valid = slot_positions()
    g = jnp.where(valid, g * (1.0 / 512.0), 0.0)
    m = m_ref[...]
    lane = lax.broadcasted_iota(jnp.int32, (1, LANES), 1)
    total = jnp.zeros((1, LANES), f32)
    decay = jnp.zeros((SLOT, LANES), f32)
    for l in range(LAYERS):
        mask = in_layer(tab_ref, l, pos)
        decay = jnp.where(mask, (1.0 - skipped(tab_ref, l)) * 0.001, decay)
        for at, square in ((l, m * m), (8 + l, g * g)):
            rows = jnp.sum(jnp.where(mask, square, 0.0), axis=0, keepdims=True)
            total = total + jnp.where(lane == at, jnp.sum(rows, axis=1, keepdims=True), 0.0)
    h = g + decay * m
    h_ref[...] = h
    row = lax.broadcasted_iota(jnp.int32, (SLOT, LANES), 0)
    out = jnp.where(row == TOUCHED, total, h)
    a = m - 0.9 * v_ref[...]
    for k in range(N_FAR):
        o_ref[k, :SLOT, :] = out
        o_ref[k, SLOT:, :] = a


def group_kernel(s_ref, n_ref):
    total = s_ref[0, TOUCHED : TOUCHED + 1, :]
    for k in range(1, N_FAR):
        total = total + s_ref[k, TOUCHED : TOUCHED + 1, :]
    n_ref[...] = jnp.broadcast_to(total[None], n_ref.shape)


def trust_at(tab_ref, trust, pos):
    lane = lax.broadcasted_iota(jnp.int32, (1, LANES), 1)
    out = jnp.zeros(pos[0].shape, f32)
    outs = [out] * len(pos)
    for l in range(LAYERS):
        one = jnp.sum(jnp.where(lane == l, trust, 0.0), axis=1, keepdims=True)
        outs = [jnp.where(in_layer(tab_ref, l, p), one, o) for p, o in zip(pos, outs)]
    return outs


def update_kernel(tab_ref, n_ref, s_ref, w_ref, t_ref, rows):
    norms = jnp.sum(n_ref[...], axis=0)
    lane = lax.broadcasted_iota(jnp.int32, (1, LANES), 1)
    skip = jnp.zeros((1, LANES), f32)
    for l in range(LAYERS):
        skip = jnp.where(lane == l, skipped(tab_ref, l), skip)
    wnorm = jnp.sqrt(norms)
    gnorm = pltpu.roll(wnorm, LANES - 8, 1)
    ratio = 0.02 * wnorm / (gnorm + 0.001 * wnorm + 1e-06)
    trust = skip + (1.0 - skip) * ratio
    t_ref[...] = trust
    at = lax.broadcasted_iota(jnp.int32, (SLOT, LANES), 0) * LANES
    at = at + lax.broadcasted_iota(jnp.int32, (SLOT, LANES), 1)
    pos = [
        at + row_of(zh * NL + lax.axis_index("zl"), q_index(), yh * NL + lax.axis_index("yl")) * LANES
        for _, zh, yh in far_slots()
    ]
    for k, t in enumerate(trust_at(tab_ref, trust, pos)):
        w = s_ref[k, SLOT:, :] - 8.0 * t * s_ref[k, :SLOT, :]
        rows[k * TOUCHED : (k + 1) * TOUCHED, :] = w[:TOUCHED, :]
    w = rows[...].astype(bf16)
    for k in range(NL * NX * NL):
        w_ref[k] = w


def own_kernel(tab_ref, t_ref, h_ref, m_ref, v_ref, om_ref, ov_ref, turn):
    shift = 2 * (NY * q_index() + y_index())
    pos, _ = slot_positions()
    (trust,) = trust_at(tab_ref, t_ref[...], [pos])
    new_v = 0.9 * v_ref[...] + 8.0 * trust * h_ref[...]
    new_m = m_ref[...] - new_v
    lane = lax.broadcasted_iota(jnp.int32, (SLOT, LANES), 1)
    for own, out in ((new_m, om_ref), (new_v, ov_ref)):
        turned = pltpu.roll(own, lax.rem(LANES - shift, LANES), 1)
        turn[:SLOT, :] = turned
        turn[SLOT:, :] = jnp.zeros((8, LANES), f32)
        out[...] = jnp.where(lane < LANES - shift, turned, turn[1 : SLOT + 1, :])


def put_core(w_ref, c, z, block, rows, tail):
    zh, zl = z // NL, z % NL
    part = NH * TOUCHED
    for x in range(NX):
        for yl in range(NL):
            peer = (zl * NX + x) * NL + yl
            block[yl * part : (yl + 1) * part, :] = w_ref[peer, zh * part : (zh + 1) * part, :].astype(f32)
        before = None
        for y in range(NY):
            at = (y % NL) * part + y // NL * TOUCHED
            base = row_of(z, x * NC, y) + c * Q_ROWS
            if before is None:
                rows[pl.ds(base, Y_ROWS), :] = block[at : at + Y_ROWS, :]
            else:
                rows[pl.ds(base, 1), :] = block[at : at + 1, :] + block[before : before + 1, :]
                rows[pl.ds(base + 1, Y_ROWS - 1), :] = block[at + 1 : at + Y_ROWS, :]
            before = at + Y_ROWS
        tail[pl.ds(z * NQ + x * NC + c, 1), :] = block[before : before + 1, :]


def own_half_kernel(w_ref, rows, tail, block):
    for z in range(NZ):
        put_core(w_ref, lax.axis_index("c"), z, block, rows, tail)


def lay_out_kernel(w_ref, rows_in, tail_in, rows, tail, o_ref, block, narrow, sems):
    copies = []
    for z in range(NZ):
        put_core(w_ref, 1 - lax.axis_index("c"), z, block, rows, tail)
        for q in range(NQ):
            last = row_of(z, q + 1, 0)
            one = tail[z * NQ + q : z * NQ + q + 1, :]
            if q + 1 < NQ:
                rows[last : last + 1, :] += one
            else:
                rows[last : last + 1, :] = one
        start, stop = z * Z_ROWS // 8 * 8, (z + 1) * Z_ROWS // 8 * 8
        narrow[start:stop, :] = rows[start:stop, :].astype(bf16)
        at = pl.ds(start, stop - start)
        copies.append(pltpu.make_async_copy(narrow.at[at], o_ref.at[at], sems.at[z]))
        copies[-1].start()
    for copy in copies:
        copy.wait()


def sent(x, axes):
    return lax.all_to_all(x, axes, 0, 0, tiled=True)


def shards(grads, master, velocity, layer_offsets, layer_sizes, lars_skip):
    tab = jnp.concatenate([layer_offsets, layer_sizes, lars_skip])
    near, far, slot = (NEAR_ROWS, LANES), (SLOT, LANES), shape(SLOT, LANES)
    sending, tab = lax.optimization_barrier((packed(grads), tab))
    spread = call(spread_kernel, shape(N_FAR, *far), [VMEM], [near])(sent(sending, NEAR))
    shared, h, m, v = call(
        owner_kernel,
        (shape(N_FAR, 2 * SLOT, LANES), slot, slot, slot),
        [SMEM] + [VMEM] * 3,
        [(SLOT + 8, LANES)],
    )(tab, sent(spread, FAR), master, velocity)
    shared = sent(shared, FAR)
    norms = call(group_kernel, shape(N_NEAR, 1, LANES), [VMEM])(shared)
    w, trust = call(
        update_kernel,
        (shape(NL * NX * NL, *near, dtype=bf16), shape(1, LANES)),
        [SMEM, VMEM, VMEM],
        [near],
    )(tab, sent(norms, NEAR), shared)
    w = sent(w, ("zl", "x", "yl"))
    other = lax.ppermute(w, "c", [(0, 1), (1, 0)])
    halves = (shape(ROWS, LANES), shape(NZ * NQ, LANES))
    block = (NL * NH * TOUCHED, LANES)
    rows, tail = call(own_half_kernel, halves, [VMEM], [block])(w)
    new_master, new_velocity = call(
        own_kernel, (slot, slot), [SMEM] + [VMEM] * 4, [(SLOT + 8, LANES)]
    )(tab, trust, h, m, v)
    _, _, weights = pl.pallas_call(
        lay_out_kernel,
        out_shape=(*halves, shape(ROWS, LANES, dtype=bf16)),
        in_specs=[VMEM] * 3,
        out_specs=(VMEM, VMEM, pl.BlockSpec(memory_space=pl.ANY)),
        input_output_aliases={1: 0, 2: 1},
        scratch_shapes=[
            pltpu.VMEM(block, f32),
            pltpu.VMEM((ROWS, LANES), bf16),
            pltpu.SemaphoreType.DMA((NZ,)),
        ],
        compiler_params=PARAMS,
    )(other, rows, tail)
    return (
        weights.reshape(ROWS * LANES),
        new_master.reshape(SLOT * LANES)[:SHARD],
        new_velocity.reshape(SLOT * LANES)[:SHARD],
    )


def solution(mesh):
    finer = Mesh(mesh.devices.reshape(NH, NL, NX, NC, NH, NL), AXES)
    owned = P(AXES)
    in_specs = (P(("zh", "zl", "x", "c"), ("yh", "yl"), None), owned, owned, P(), P(), P())
    return jax.shard_map(
        shards, mesh=finer, in_specs=in_specs, out_specs=(P(), owned, owned), check_vma=False
    )
```

```python
import jax
import jax.numpy as jnp
from jax import lax
from jax.experimental import pallas as pl
from jax.experimental.pallas import tpu as pltpu
from jax.sharding import Mesh
from jax.sharding import PartitionSpec as P

AXES = ("zh", "zl", "xh", "xl", "c", "yh", "yl")
NEAR = ("zl", "xh", "xl", "c", "yl")
FAR = ("zh", "yh")
WIDE = ("zh", "xh", "yh")
NX, NC, NL, NH = 4, 2, 2, 4
NY, NZ = NH * NL, NH * NL
NQ = NX * NC
N_NEAR, N_FAR = NL * NQ * NL, NH * NH
LANES = 128
SHARD = 1666
ROWS = 6664
Z_ROWS = ROWS // NZ
Q_ROWS = 104
Y_ROWS = 13
TOUCHED = 14
SLOT = 16
NEAR_ROWS = N_FAR * TOUCHED
NXH = NX // 2
N_CUBE, N_WIDE = 8, NH * NXH * NH
HALF_ROWS = N_WIDE * TOUCHED
LAYERS = 6
STEPS = 7
STEP_ROWS = ROWS // STEPS
CHUNK = 136
f32 = jnp.float32
bf16 = jnp.bfloat16
VMEM = pl.BlockSpec(memory_space=pltpu.VMEM)
SMEM = pl.BlockSpec(memory_space=pltpu.SMEM)
PARAMS = pltpu.CompilerParams(vmem_limit_bytes=40 * 1024 * 1024)


def shape(*dims, dtype=f32):
    return jax.ShapeDtypeStruct(dims, dtype)


def call(kernel, out_shape, ins, scratch=()):
    many = isinstance(out_shape, tuple)
    return pl.pallas_call(
        kernel,
        out_shape=out_shape,
        in_specs=list(ins),
        out_specs=(VMEM,) * len(out_shape) if many else VMEM,
        scratch_shapes=[pltpu.VMEM(s, f32) for s in scratch],
        compiler_params=PARAMS,
    )


def row_of(z, q, y):
    return z * Z_ROWS + q * Q_ROWS + y * Y_ROWS


def z_index():
    return lax.axis_index("zh") * NL + lax.axis_index("zl")


def q_index():
    return (lax.axis_index("xh") * 2 + lax.axis_index("xl")) * NC + lax.axis_index("c")


def y_index():
    return lax.axis_index("yh") * NL + lax.axis_index("yl")


def far_slots():
    return [(k, k // NH, k % NH) for k in range(N_FAR)]


def pack_kernel(x_ref, o_ref, held, sems, wide, rows):
    copies = []
    for i in range(STEPS):
        at = pl.ds(i * STEP_ROWS, STEP_ROWS)
        copies.append(pltpu.make_async_copy(x_ref.at[at], held.at[at], sems.at[i]))
        copies[-1].start()
    for i in range(STEPS):
        copies[i].wait()

        def widen(k, _):
            at = i * STEP_ROWS + k * CHUNK
            for r in range(CHUNK):
                wide[pl.ds(at + r, 1), :] = held[at + r].astype(f32)
            return _

        lax.fori_loop(0, STEP_ROWS // CHUNK, widen, 0)
    for label in range(N_CUBE):
        zl, xl, yl = label // 4, label // 2 % 2, label % 2
        for k in range(NC * N_WIDE):
            c, zh, xh, yh = k // N_WIDE, k // (NXH * NH) % NH, k // NH % NXH, k % NH
            base = row_of(zh * NL + zl, (xh * 2 + xl) * NC + c, yh * NL + yl)
            rows[k * TOUCHED : (k + 1) * TOUCHED, :] = wide[base : base + TOUCHED, :]
        o_ref[label] = rows[...].astype(bf16)


def packed(grads):
    return pl.pallas_call(
        pack_kernel,
        out_shape=shape(N_CUBE, NC * HALF_ROWS, LANES, dtype=bf16),
        in_specs=[pl.BlockSpec(memory_space=pl.ANY)],
        out_specs=VMEM,
        scratch_shapes=[
            pltpu.VMEM((ROWS, 1, LANES), bf16),
            pltpu.SemaphoreType.DMA((STEPS,)),
            pltpu.VMEM((ROWS, LANES), f32),
            pltpu.VMEM((NC * HALF_ROWS, LANES), f32),
        ],
        compiler_params=pltpu.CompilerParams(vmem_limit_bytes=51 * 1024 * 1024),
    )(grads.reshape(ROWS, 1, LANES))


def cubes():
    def pair(k, parity, count, c):
        return (2 * k + 2 * c * (1 - parity) + parity) % count

    groups = []
    for c in range(NC):
        for kz in range(NZ // 2):
            for kx in range(NX // 2):
                for ky in range(NY // 2):
                    group = []
                    for label in range(N_CUBE):
                        z = pair(kz, label // 4, NZ, c)
                        x = pair(kx, label // 2 % 2, NX, c)
                        y = pair(ky, label % 2, NY, c)
                        group.append(((z * NX + x) * NC + c) * NY + y)
                    groups.append(group)
    return groups


def halve_kernel(r_ref, keep_ref, give_ref, rows):
    total = r_ref[0].astype(f32)
    for k in range(1, N_CUBE):
        total = total + r_ref[k].astype(f32)
    rows[...] = total
    c = lax.axis_index("c")
    keep_ref[...] = rows[pl.ds(pl.multiple_of(c * HALF_ROWS, 8), HALF_ROWS), :]
    give_ref[...] = rows[pl.ds(pl.multiple_of((1 - c) * HALF_ROWS, 8), HALF_ROWS), :]


def spread_kernel(a_ref, b_ref, o_ref, rows):
    rows[...] = a_ref[...] + b_ref[...]
    for k in range(N_WIDE):
        o_ref[k, :TOUCHED, :] = rows[k * TOUCHED : (k + 1) * TOUCHED, :]
        o_ref[k, TOUCHED:, :] = jnp.zeros((SLOT - TOUCHED, LANES), f32)


def slot_positions():
    q, y = q_index(), y_index()
    owner = (z_index() * NQ + q) * NY + y
    row = lax.broadcasted_iota(jnp.int32, (SLOT, LANES), 0)
    lane = lax.broadcasted_iota(jnp.int32, (SLOT, LANES), 1)
    local = row * LANES + lane - 2 * (NY * q + y)
    return local + owner * SHARD, (local >= 0) & (local < SHARD)


def in_layer(tab_ref, l, pos):
    start = tab_ref[l]
    return (pos >= start) & (pos < start + tab_ref[LAYERS + l])


def skipped(tab_ref, l):
    return tab_ref[2 * LAYERS + l].astype(f32)


def placed(flat_ref, rows):
    whole = SHARD // LANES
    rows[...] = jnp.zeros((SLOT + 8, LANES), f32)
    for k in range(whole):
        rows[8 + k, :] = flat_ref[pl.ds(k * LANES, LANES)]
    rows[8 + whole, pl.ds(0, SHARD - whole * LANES)] = flat_ref[pl.ds(whole * LANES, SHARD - whole * LANES)]
    shift = 2 * (NY * q_index() + y_index())
    lane = lax.broadcasted_iota(jnp.int32, (SLOT, LANES), 1)
    here = pltpu.roll(rows[8:, :], shift, 1)
    above = pltpu.roll(rows[7 : SLOT + 7, :], shift, 1)
    return jnp.where(lane >= shift, here, above)


def owner_kernel(tab_ref, r_ref, mf_ref, vf_ref, o_ref, h_ref, m_ref, v_ref, rows):
    m_ref[...] = placed(mf_ref, rows)
    v_ref[...] = placed(vf_ref, rows)
    g = r_ref[0]
    for k in range(1, N_WIDE):
        g = g + r_ref[k]
    pos, valid = slot_positions()
    g = jnp.where(valid, g * (1.0 / 512.0), 0.0)
    m = m_ref[...]
    lane = lax.broadcasted_iota(jnp.int32, (1, LANES), 1)
    total = jnp.zeros((1, LANES), f32)
    decay = jnp.zeros((SLOT, LANES), f32)
    for l in range(LAYERS):
        mask = in_layer(tab_ref, l, pos)
        decay = jnp.where(mask, (1.0 - skipped(tab_ref, l)) * 0.001, decay)
        for at, square in ((l, m * m), (8 + l, g * g)):
            rows = jnp.sum(jnp.where(mask, square, 0.0), axis=0, keepdims=True)
            total = total + jnp.where(lane == at, jnp.sum(rows, axis=1, keepdims=True), 0.0)
    h = g + decay * m
    h_ref[...] = h
    row = lax.broadcasted_iota(jnp.int32, (SLOT, LANES), 0)
    out = jnp.where(row == TOUCHED, total, h)
    a = m - 0.9 * v_ref[...]
    for k in range(N_FAR):
        o_ref[k, :SLOT, :] = out
        o_ref[k, SLOT:, :] = a


def group_kernel(s_ref, n_ref):
    total = s_ref[0, TOUCHED : TOUCHED + 1, :]
    for k in range(1, N_FAR):
        total = total + s_ref[k, TOUCHED : TOUCHED + 1, :]
    n_ref[...] = jnp.broadcast_to(total[None], n_ref.shape)


def trust_at(tab_ref, trust, pos):
    lane = lax.broadcasted_iota(jnp.int32, (1, LANES), 1)
    out = jnp.zeros(pos[0].shape, f32)
    outs = [out] * len(pos)
    for l in range(LAYERS):
        one = jnp.sum(jnp.where(lane == l, trust, 0.0), axis=1, keepdims=True)
        outs = [jnp.where(in_layer(tab_ref, l, p), one, o) for p, o in zip(pos, outs)]
    return outs


def update_kernel(tab_ref, n_ref, s_ref, w_ref, t_ref, rows):
    norms = jnp.sum(n_ref[...], axis=0)
    lane = lax.broadcasted_iota(jnp.int32, (1, LANES), 1)
    skip = jnp.zeros((1, LANES), f32)
    for l in range(LAYERS):
        skip = jnp.where(lane == l, skipped(tab_ref, l), skip)
    wnorm = jnp.sqrt(norms)
    gnorm = pltpu.roll(wnorm, LANES - 8, 1)
    ratio = 0.02 * wnorm / (gnorm + 0.001 * wnorm + 1e-06)
    trust = skip + (1.0 - skip) * ratio
    t_ref[...] = trust
    at = lax.broadcasted_iota(jnp.int32, (SLOT, LANES), 0) * LANES
    at = at + lax.broadcasted_iota(jnp.int32, (SLOT, LANES), 1)
    pos = [
        at + row_of(zh * NL + lax.axis_index("zl"), q_index(), yh * NL + lax.axis_index("yl")) * LANES
        for _, zh, yh in far_slots()
    ]
    for k, t in enumerate(trust_at(tab_ref, trust, pos)):
        w = s_ref[k, SLOT:, :] - 8.0 * t * s_ref[k, :SLOT, :]
        rows[k * TOUCHED : (k + 1) * TOUCHED, :] = w[:TOUCHED, :]
    w = rows[...].astype(bf16)
    for k in range(NL * NX * NL):
        w_ref[k] = w


def own_kernel(tab_ref, t_ref, h_ref, m_ref, v_ref, om_ref, ov_ref, turn):
    shift = 2 * (NY * q_index() + y_index())
    pos, _ = slot_positions()
    (trust,) = trust_at(tab_ref, t_ref[...], [pos])
    new_v = 0.9 * v_ref[...] + 8.0 * trust * h_ref[...]
    new_m = m_ref[...] - new_v
    lane = lax.broadcasted_iota(jnp.int32, (SLOT, LANES), 1)
    for own, out in ((new_m, om_ref), (new_v, ov_ref)):
        turned = pltpu.roll(own, lax.rem(LANES - shift, LANES), 1)
        turn[:SLOT, :] = turned
        turn[SLOT:, :] = jnp.zeros((8, LANES), f32)
        out[...] = jnp.where(lane < LANES - shift, turned, turn[1 : SLOT + 1, :])


def put_core(w_ref, c, z, block, rows, tail):
    zh, zl = z // NL, z % NL
    part = NH * TOUCHED
    for x in range(NX):
        for yl in range(NL):
            peer = (zl * NX + x) * NL + yl
            block[yl * part : (yl + 1) * part, :] = w_ref[peer, zh * part : (zh + 1) * part, :].astype(f32)
        before = None
        for y in range(NY):
            at = (y % NL) * part + y // NL * TOUCHED
            base = row_of(z, x * NC, y) + c * Q_ROWS
            if before is None:
                rows[pl.ds(base, Y_ROWS), :] = block[at : at + Y_ROWS, :]
            else:
                rows[pl.ds(base, 1), :] = block[at : at + 1, :] + block[before : before + 1, :]
                rows[pl.ds(base + 1, Y_ROWS - 1), :] = block[at + 1 : at + Y_ROWS, :]
            before = at + Y_ROWS
        tail[pl.ds(z * NQ + x * NC + c, 1), :] = block[before : before + 1, :]


def own_half_kernel(w_ref, rows, tail, block):
    for z in range(NZ):
        put_core(w_ref, lax.axis_index("c"), z, block, rows, tail)


def lay_out_kernel(w_ref, rows_in, tail_in, rows, tail, o_ref, block, narrow, sems):
    copies = []
    for z in range(NZ):
        put_core(w_ref, 1 - lax.axis_index("c"), z, block, rows, tail)
        for q in range(NQ):
            last = row_of(z, q + 1, 0)
            one = tail[z * NQ + q : z * NQ + q + 1, :]
            if q + 1 < NQ:
                rows[last : last + 1, :] += one
            else:
                rows[last : last + 1, :] = one
        start, stop = z * Z_ROWS // 8 * 8, (z + 1) * Z_ROWS // 8 * 8
        narrow[start:stop, :] = rows[start:stop, :].astype(bf16)
        at = pl.ds(start, stop - start)
        copies.append(pltpu.make_async_copy(narrow.at[at], o_ref.at[at], sems.at[z]))
        copies[-1].start()
    for copy in copies:
        copy.wait()


def sent(x, axes):
    return lax.all_to_all(x, axes, 0, 0, tiled=True)


def swapped(x):
    return lax.ppermute(x, "c", [(0, 1), (1, 0)])


def shards(grads, master, velocity, layer_offsets, layer_sizes, lars_skip):
    tab = jnp.concatenate([layer_offsets, layer_sizes, lars_skip])
    near, far, slot = (NEAR_ROWS, LANES), (SLOT, LANES), shape(SLOT, LANES)
    sending, tab = lax.optimization_barrier((packed(grads), tab))
    received = lax.all_to_all(sending, AXES, 0, 0, axis_index_groups=cubes(), tiled=True)
    half = (HALF_ROWS, LANES)
    keep, give = call(
        halve_kernel, (shape(*half), shape(*half)), [VMEM], [(NC * HALF_ROWS, LANES)]
    )(received)
    spread = call(spread_kernel, shape(N_WIDE, *far), [VMEM, VMEM], [half])(keep, swapped(give))
    shared, h, m, v = call(
        owner_kernel,
        (shape(N_FAR, 2 * SLOT, LANES), slot, slot, slot),
        [SMEM] + [VMEM] * 3,
        [(SLOT + 8, LANES)],
    )(tab, sent(spread, WIDE), master, velocity)
    shared = sent(shared, FAR)
    norms = call(group_kernel, shape(N_NEAR, 1, LANES), [VMEM])(shared)
    w, trust = call(
        update_kernel,
        (shape(NL * NX * NL, *near, dtype=bf16), shape(1, LANES)),
        [SMEM, VMEM, VMEM],
        [near],
    )(tab, sent(norms, NEAR), shared)
    w = sent(w, ("zl", "xh", "xl", "yl"))
    other = swapped(w)
    halves = (shape(ROWS, LANES), shape(NZ * NQ, LANES))
    block = (NL * NH * TOUCHED, LANES)
    rows, tail = call(own_half_kernel, halves, [VMEM], [block])(w)
    new_master, new_velocity = call(
        own_kernel, (slot, slot), [SMEM] + [VMEM] * 4, [(SLOT + 8, LANES)]
    )(tab, trust, h, m, v)
    _, _, weights = pl.pallas_call(
        lay_out_kernel,
        out_shape=(*halves, shape(ROWS, LANES, dtype=bf16)),
        in_specs=[VMEM] * 3,
        out_specs=(VMEM, VMEM, pl.BlockSpec(memory_space=pl.ANY)),
        input_output_aliases={1: 0, 2: 1},
        scratch_shapes=[
            pltpu.VMEM(block, f32),
            pltpu.VMEM((ROWS, LANES), bf16),
            pltpu.SemaphoreType.DMA((NZ,)),
        ],
        compiler_params=PARAMS,
    )(other, rows, tail)
    return (
        weights.reshape(ROWS * LANES),
        new_master.reshape(SLOT * LANES)[:SHARD],
        new_velocity.reshape(SLOT * LANES)[:SHARD],
    )


def solution(mesh):
    finer = Mesh(mesh.devices.reshape(NH, NL, NXH, 2, NC, NH, NL), AXES)
    owned = P(AXES)
    in_specs = (P(("zh", "zl", "xh", "xl", "c"), ("yh", "yl"), None), owned, owned, P(), P(), P())
    return jax.shard_map(
        shards, mesh=finer, in_specs=in_specs, out_specs=(P(), owned, owned), check_vma=False
    )
```

```python
import functools

import jax
import jax.numpy as jnp
from jax import lax
from jax.experimental import pallas as pl
from jax.experimental.pallas import tpu as pltpu
from jax.sharding import Mesh
from jax.sharding import PartitionSpec as P

AXES = ("zh", "zl", "xh", "xl", "c", "yh", "yl")
NEAR = ("zl", "xh", "xl", "c", "yl")
FAR = ("zh", "yh")
WIDE = ("zh", "xh", "yh")
NX, NC, NL, NH = 4, 2, 2, 4
NY, NZ = NH * NL, NH * NL
NQ = NX * NC
N_NEAR, N_FAR = NL * NQ * NL, NH * NH
LANES = 128
SHARD = 1666
ROWS = 6664
Z_ROWS = ROWS // NZ
Q_ROWS = 104
Y_ROWS = 13
TOUCHED = 14
SLOT = 16
NEAR_ROWS = N_FAR * TOUCHED
NXH = NX // 2
N_CUBE, N_WIDE = 8, NH * NXH * NH
HALF_ROWS = N_WIDE * TOUCHED
LAYERS = 6
STEPS = 7
STEP_ROWS = ROWS // STEPS
CHUNK = 136
f32 = jnp.float32
bf16 = jnp.bfloat16
VMEM = pl.BlockSpec(memory_space=pltpu.VMEM)
SMEM = pl.BlockSpec(memory_space=pltpu.SMEM)
PARAMS = pltpu.CompilerParams(vmem_limit_bytes=40 * 1024 * 1024)


def shape(*dims, dtype=f32):
    return jax.ShapeDtypeStruct(dims, dtype)


def call(kernel, out_shape, ins, scratch=()):
    many = isinstance(out_shape, tuple)
    return pl.pallas_call(
        kernel,
        out_shape=out_shape,
        in_specs=list(ins),
        out_specs=(VMEM,) * len(out_shape) if many else VMEM,
        scratch_shapes=[pltpu.VMEM(s, f32) for s in scratch],
        compiler_params=PARAMS,
    )


def row_of(z, q, y):
    return z * Z_ROWS + q * Q_ROWS + y * Y_ROWS


def z_index():
    return lax.axis_index("zh") * NL + lax.axis_index("zl")


def q_index():
    return (lax.axis_index("xh") * 2 + lax.axis_index("xl")) * NC + lax.axis_index("c")


def y_index():
    return lax.axis_index("yh") * NL + lax.axis_index("yl")


def far_slots():
    return [(k, k // NH, k % NH) for k in range(N_FAR)]


def pack_kernel(x_ref, o_ref, held, sems, wide, rows):
    copies = []
    for i in range(STEPS):
        at = pl.ds(i * STEP_ROWS, STEP_ROWS)
        copies.append(pltpu.make_async_copy(x_ref.at[at], held.at[at], sems.at[i]))
        copies[-1].start()
    for i in range(STEPS):
        copies[i].wait()

        def widen(k, _):
            at = i * STEP_ROWS + k * CHUNK
            for r in range(CHUNK):
                wide[pl.ds(at + r, 1), :] = held[at + r].astype(f32)
            return _

        lax.fori_loop(0, STEP_ROWS // CHUNK, widen, 0)
    for label in range(N_CUBE):
        zl, xl, yl = label // 4, label // 2 % 2, label % 2
        for k in range(NC * N_WIDE):
            c, zh, xh, yh = k // N_WIDE, k // (NXH * NH) % NH, k // NH % NXH, k % NH
            base = row_of(zh * NL + zl, (xh * 2 + xl) * NC + c, yh * NL + yl)
            rows[k * TOUCHED : (k + 1) * TOUCHED, :] = wide[base : base + TOUCHED, :]
        o_ref[label] = rows[...].astype(bf16)


def packed(grads):
    return pl.pallas_call(
        pack_kernel,
        out_shape=shape(N_CUBE, NC * HALF_ROWS, LANES, dtype=bf16),
        in_specs=[pl.BlockSpec(memory_space=pl.ANY)],
        out_specs=VMEM,
        scratch_shapes=[
            pltpu.VMEM((ROWS, 1, LANES), bf16),
            pltpu.SemaphoreType.DMA((STEPS,)),
            pltpu.VMEM((ROWS, LANES), f32),
            pltpu.VMEM((NC * HALF_ROWS, LANES), f32),
        ],
        compiler_params=pltpu.CompilerParams(vmem_limit_bytes=51 * 1024 * 1024),
    )(grads.reshape(ROWS, 1, LANES))


def cubes():
    def pair(k, parity, count, shifted):
        return (2 * k + 2 * shifted * (1 - parity) + parity) % count

    groups = []
    for c in range(NC):
        for kz in range(NZ // 2):
            for kx in range(NX // 2):
                for ky in range(NY // 2):
                    group = []
                    for label in range(N_CUBE):
                        z = pair(kz, label // 4, NZ, c)
                        x = pair(kx, label // 2 % 2, NX, c)
                        y = pair(ky, label % 2, NY, 1 - c)
                        group.append(((z * NX + x) * NC + c) * NY + y)
                    groups.append(group)
    return groups


def half_kernel(mine, r_ref, o_ref):
    c = lax.axis_index("c")
    c = c if mine else 1 - c
    at = pl.ds(pl.multiple_of(c * HALF_ROWS, 16), HALF_ROWS)
    total = r_ref[0, at, :].astype(f32)
    for k in range(1, N_CUBE):
        total = total + r_ref[k, at, :].astype(f32)
    o_ref[...] = total


def spread_kernel(a_ref, b_ref, o_ref, rows):
    rows[...] = a_ref[...] + b_ref[...]
    for k in range(N_WIDE):
        o_ref[k, :TOUCHED, :] = rows[k * TOUCHED : (k + 1) * TOUCHED, :]
        o_ref[k, TOUCHED:, :] = jnp.zeros((SLOT - TOUCHED, LANES), f32)


def slot_positions():
    q, y = q_index(), y_index()
    owner = (z_index() * NQ + q) * NY + y
    row = lax.broadcasted_iota(jnp.int32, (SLOT, LANES), 0)
    lane = lax.broadcasted_iota(jnp.int32, (SLOT, LANES), 1)
    local = row * LANES + lane - 2 * (NY * q + y)
    return local + owner * SHARD, (local >= 0) & (local < SHARD)


def in_layer(tab_ref, l, pos):
    start = tab_ref[l]
    return (pos >= start) & (pos < start + tab_ref[LAYERS + l])


def skipped(tab_ref, l):
    return tab_ref[2 * LAYERS + l].astype(f32)


def placed(flat_ref, rows):
    whole = SHARD // LANES
    rows[...] = jnp.zeros((SLOT + 8, LANES), f32)
    for k in range(whole):
        rows[8 + k, :] = flat_ref[pl.ds(k * LANES, LANES)]
    rows[8 + whole, pl.ds(0, SHARD - whole * LANES)] = flat_ref[pl.ds(whole * LANES, SHARD - whole * LANES)]
    shift = 2 * (NY * q_index() + y_index())
    lane = lax.broadcasted_iota(jnp.int32, (SLOT, LANES), 1)
    here = pltpu.roll(rows[8:, :], shift, 1)
    above = pltpu.roll(rows[7 : SLOT + 7, :], shift, 1)
    return jnp.where(lane >= shift, here, above)


def owner_kernel(tab_ref, r_ref, mf_ref, vf_ref, o_ref, h_ref, m_ref, v_ref, turn):
    m_ref[...] = placed(mf_ref, turn)
    v_ref[...] = placed(vf_ref, turn)
    g = r_ref[0]
    for k in range(1, N_WIDE):
        g = g + r_ref[k]
    pos, valid = slot_positions()
    g = jnp.where(valid, g * (1.0 / 512.0), 0.0)
    m = m_ref[...]
    row = lax.broadcasted_iota(jnp.int32, (SLOT, LANES), 0)
    lane = lax.broadcasted_iota(jnp.int32, (SLOT, LANES), 1)
    stack = jnp.zeros((SLOT, LANES), f32)
    decay = jnp.zeros((SLOT, LANES), f32)
    mm, gg = m * m, g * g
    for l in range(LAYERS):
        mask = in_layer(tab_ref, l, pos)
        decay = jnp.where(mask, (1.0 - skipped(tab_ref, l)) * 0.001, decay)
        for at, square in ((l, mm), (8 + l, gg)):
            rows = jnp.sum(jnp.where(mask, square, 0.0), axis=0, keepdims=True)
            stack = jnp.where(row == at, rows, stack)
    sums = jnp.sum(stack, axis=1, keepdims=True)
    total = jnp.sum(jnp.where(lane == row, sums, 0.0), axis=0, keepdims=True)
    h = g + decay * m
    h_ref[...] = h
    out = jnp.where(row == TOUCHED, total, h)
    a = m - 0.9 * v_ref[...]
    for k in range(N_FAR):
        o_ref[k, :SLOT, :] = out
        o_ref[k, SLOT:, :] = a


def group_kernel(s_ref, n_ref):
    total = s_ref[0, TOUCHED : TOUCHED + 1, :]
    for k in range(1, N_FAR):
        total = total + s_ref[k, TOUCHED : TOUCHED + 1, :]
    n_ref[...] = jnp.broadcast_to(total[None], n_ref.shape)


def trust_at(tab_ref, trust, pos):
    lane = lax.broadcasted_iota(jnp.int32, (1, LANES), 1)
    out = jnp.zeros(pos[0].shape, f32)
    outs = [out] * len(pos)
    for l in range(LAYERS):
        one = jnp.sum(jnp.where(lane == l, trust, 0.0), axis=1, keepdims=True)
        outs = [jnp.where(in_layer(tab_ref, l, p), one, o) for p, o in zip(pos, outs)]
    return outs


def update_kernel(tab_ref, n_ref, s_ref, w_ref, t_ref, rows):
    norms = jnp.sum(n_ref[...], axis=0)
    lane = lax.broadcasted_iota(jnp.int32, (1, LANES), 1)
    skip = jnp.zeros((1, LANES), f32)
    for l in range(LAYERS):
        skip = jnp.where(lane == l, skipped(tab_ref, l), skip)
    wnorm = jnp.sqrt(norms)
    gnorm = pltpu.roll(wnorm, LANES - 8, 1)
    ratio = 0.02 * wnorm / (gnorm + 0.001 * wnorm + 1e-06)
    trust = skip + (1.0 - skip) * ratio
    t_ref[...] = trust
    at = lax.broadcasted_iota(jnp.int32, (SLOT, LANES), 0) * LANES
    at = at + lax.broadcasted_iota(jnp.int32, (SLOT, LANES), 1)
    pos = [
        at + row_of(zh * NL + lax.axis_index("zl"), q_index(), yh * NL + lax.axis_index("yl")) * LANES
        for _, zh, yh in far_slots()
    ]
    for k, t in enumerate(trust_at(tab_ref, trust, pos)):
        w = s_ref[k, SLOT:, :] - 8.0 * t * s_ref[k, :SLOT, :]
        rows[k * TOUCHED : (k + 1) * TOUCHED, :] = w[:TOUCHED, :]
    w = rows[...].astype(bf16)
    for k in range(NL * NX * NL):
        w_ref[k] = w


def own_kernel(tab_ref, t_ref, h_ref, m_ref, v_ref, om_ref, ov_ref, turn):
    shift = 2 * (NY * q_index() + y_index())
    pos, _ = slot_positions()
    (trust,) = trust_at(tab_ref, t_ref[...], [pos])
    new_v = 0.9 * v_ref[...] + 8.0 * trust * h_ref[...]
    new_m = m_ref[...] - new_v
    lane = lax.broadcasted_iota(jnp.int32, (SLOT, LANES), 1)
    for own, out in ((new_m, om_ref), (new_v, ov_ref)):
        turned = pltpu.roll(own, lax.rem(LANES - shift, LANES), 1)
        turn[:SLOT, :] = turned
        turn[SLOT:, :] = jnp.zeros((8, LANES), f32)
        out[...] = jnp.where(lane < LANES - shift, turned, turn[1 : SLOT + 1, :])


def put_core(w_ref, c, z, block, rows, tail):
    zh, zl = z // NL, z % NL
    part = NH * TOUCHED
    for x in range(NX):
        for yl in range(NL):
            peer = (zl * NX + x) * NL + yl
            block[yl * part : (yl + 1) * part, :] = w_ref[peer, zh * part : (zh + 1) * part, :].astype(f32)
        before = None
        for y in range(NY):
            at = (y % NL) * part + y // NL * TOUCHED
            base = row_of(z, x * NC, y) + c * Q_ROWS
            if before is None:
                rows[pl.ds(base, Y_ROWS), :] = block[at : at + Y_ROWS, :]
            else:
                rows[pl.ds(base, 1), :] = block[at : at + 1, :] + block[before : before + 1, :]
                rows[pl.ds(base + 1, Y_ROWS - 1), :] = block[at + 1 : at + Y_ROWS, :]
            before = at + Y_ROWS
        tail[pl.ds(z * NQ + x * NC + c, 1), :] = block[before : before + 1, :]


def own_half_kernel(w_ref, rows, tail, block):
    for z in range(NZ):
        put_core(w_ref, lax.axis_index("c"), z, block, rows, tail)


def lay_out_kernel(w_ref, rows_in, tail_in, rows, tail, o_ref, block, narrow, sems):
    copies = []
    for z in range(NZ):
        put_core(w_ref, 1 - lax.axis_index("c"), z, block, rows, tail)
        for q in range(NQ):
            last = row_of(z, q + 1, 0)
            one = tail[z * NQ + q : z * NQ + q + 1, :]
            if q + 1 < NQ:
                rows[last : last + 1, :] += one
            else:
                rows[last : last + 1, :] = one
        start, stop = z * Z_ROWS // 8 * 8, (z + 1) * Z_ROWS // 8 * 8
        narrow[start:stop, :] = rows[start:stop, :].astype(bf16)
        at = pl.ds(start, stop - start)
        copies.append(pltpu.make_async_copy(narrow.at[at], o_ref.at[at], sems.at[z]))
        copies[-1].start()
    for copy in copies:
        copy.wait()


def sent(x, axes):
    return lax.all_to_all(x, axes, 0, 0, tiled=True)


def swapped(x):
    return lax.ppermute(x, "c", [(0, 1), (1, 0)])


def shards(grads, master, velocity, layer_offsets, layer_sizes, lars_skip):
    tab = jnp.concatenate([layer_offsets, layer_sizes, lars_skip])
    near, far, slot = (NEAR_ROWS, LANES), (SLOT, LANES), shape(SLOT, LANES)
    sending, tab = lax.optimization_barrier((packed(grads), tab))
    received = lax.all_to_all(sending, AXES, 0, 0, axis_index_groups=cubes(), tiled=True)
    half = (HALF_ROWS, LANES)
    give = swapped(call(functools.partial(half_kernel, False), shape(*half), [VMEM])(received))
    keep = call(functools.partial(half_kernel, True), shape(*half), [VMEM])(received)
    spread = call(spread_kernel, shape(N_WIDE, *far), [VMEM, VMEM], [half])(keep, give)
    shared, h, m, v = call(
        owner_kernel,
        (shape(N_FAR, 2 * SLOT, LANES), slot, slot, slot),
        [SMEM] + [VMEM] * 3,
        [(SLOT + 8, LANES)],
    )(tab, sent(spread, WIDE), master, velocity)
    shared = sent(shared, FAR)
    norms = call(group_kernel, shape(N_NEAR, 1, LANES), [VMEM])(shared)
    w, trust = call(
        update_kernel,
        (shape(NL * NX * NL, *near, dtype=bf16), shape(1, LANES)),
        [SMEM, VMEM, VMEM],
        [near],
    )(tab, sent(norms, NEAR), shared)
    w = sent(w, ("zl", "xh", "xl", "yl"))
    other = swapped(w)
    halves = (shape(ROWS, LANES), shape(NZ * NQ, LANES))
    block = (NL * NH * TOUCHED, LANES)
    rows, tail = call(own_half_kernel, halves, [VMEM], [block])(w)
    new_master, new_velocity = call(
        own_kernel, (slot, slot), [SMEM] + [VMEM] * 4, [(SLOT + 8, LANES)]
    )(tab, trust, h, m, v)
    _, _, weights = pl.pallas_call(
        lay_out_kernel,
        out_shape=(*halves, shape(ROWS, LANES, dtype=bf16)),
        in_specs=[VMEM] * 3,
        out_specs=(VMEM, VMEM, pl.BlockSpec(memory_space=pl.ANY)),
        input_output_aliases={1: 0, 2: 1},
        scratch_shapes=[
            pltpu.VMEM(block, f32),
            pltpu.VMEM((ROWS, LANES), bf16),
            pltpu.SemaphoreType.DMA((NZ,)),
        ],
        compiler_params=PARAMS,
    )(other, rows, tail)
    return (
        weights.reshape(ROWS * LANES),
        new_master.reshape(SLOT * LANES)[:SHARD],
        new_velocity.reshape(SLOT * LANES)[:SHARD],
    )


def solution(mesh):
    finer = Mesh(mesh.devices.reshape(NH, NL, NXH, 2, NC, NH, NL), AXES)
    owned = P(AXES)
    in_specs = (P(("zh", "zl", "xh", "xl", "c"), ("yh", "yl"), None), owned, owned, P(), P(), P())
    return jax.shard_map(
        shards, mesh=finer, in_specs=in_specs, out_specs=(P(), owned, owned), check_vma=False
    )
```

```python
import functools

import jax
import jax.numpy as jnp
from jax import lax
from jax.experimental import pallas as pl
from jax.experimental.pallas import tpu as pltpu
from jax.sharding import Mesh
from jax.sharding import PartitionSpec as P

AXES = ("zh", "zl", "xh", "xl", "c", "yh", "yl")
NEAR = ("zl", "xh", "xl", "c", "yl")
FAR = ("zh", "yh")
WIDE = ("zh", "xh", "yh")
NX, NC, NL, NH = 4, 2, 2, 4
NY, NZ = NH * NL, NH * NL
NQ = NX * NC
N_NEAR, N_FAR = NL * NQ * NL, NH * NH
LANES = 128
SHARD = 1666
ROWS = 6664
Z_ROWS = ROWS // NZ
Q_ROWS = 104
Y_ROWS = 13
TOUCHED = 14
SLOT = 16
NEAR_ROWS = N_FAR * TOUCHED
NXH = NX // 2
N_CUBE, N_WIDE = 8, NH * NXH * NH
HALF_ROWS = N_WIDE * TOUCHED
LAYERS = 6
CHUNK = 136
STEPS = (2, 5, 7, 7, 7, 7, 7, 7)
SPARE = 8
f32 = jnp.float32
bf16 = jnp.bfloat16
VMEM = pl.BlockSpec(memory_space=pltpu.VMEM)
SMEM = pl.BlockSpec(memory_space=pltpu.SMEM)
PARAMS = pltpu.CompilerParams(vmem_limit_bytes=40 * 1024 * 1024)


def shape(*dims, dtype=f32):
    return jax.ShapeDtypeStruct(dims, dtype)


def call(kernel, out_shape, ins, scratch=()):
    many = isinstance(out_shape, tuple)
    return pl.pallas_call(
        kernel,
        out_shape=out_shape,
        in_specs=list(ins),
        out_specs=(VMEM,) * len(out_shape) if many else VMEM,
        scratch_shapes=[pltpu.VMEM(s, f32) for s in scratch],
        compiler_params=PARAMS,
    )


def row_of(z, q, y):
    return z * Z_ROWS + q * Q_ROWS + y * Y_ROWS


def z_index():
    return lax.axis_index("zh") * NL + lax.axis_index("zl")


def q_index():
    return (lax.axis_index("xh") * 2 + lax.axis_index("xl")) * NC + lax.axis_index("c")


def y_index():
    return lax.axis_index("yh") * NL + lax.axis_index("yl")


def far_slots():
    return [(k, k // NH, k % NH) for k in range(N_FAR)]


def pack_kernel(x_ref, o_ref, held, sems, wide, rows):
    copies, starts = [], [CHUNK * sum(STEPS[:i]) for i in range(len(STEPS))]
    for i, count in enumerate(STEPS):
        at = pl.ds(starts[i], count * CHUNK)
        copies.append(pltpu.make_async_copy(x_ref.at[at], held.at[at], sems.at[i]))
        copies[-1].start()
    for i, count in enumerate(STEPS):
        copies[i].wait()

        def widen(k, _):
            at = starts[i] + k * CHUNK
            for r in range(CHUNK):
                wide[pl.ds(at + r, 1), :] = held[at + r].astype(f32)
            return _

        lax.fori_loop(0, count, widen, 0)
    for label in range(N_CUBE):
        zl, xl, yl = label // 4, label // 2 % 2, label % 2
        for k in range(NC * N_WIDE):
            c, zh, xh, yh = k // N_WIDE, k // (NXH * NH) % NH, k // NH % NXH, k % NH
            base = row_of(zh * NL + zl, (xh * 2 + xl) * NC + c, yh * NL + yl)
            rows[k * TOUCHED : (k + 1) * TOUCHED, :] = wide[base : base + TOUCHED, :]
        o_ref[label] = rows[: NC * HALF_ROWS, :].astype(bf16)


def packed(grads):
    return pl.pallas_call(
        pack_kernel,
        out_shape=shape(N_CUBE, NC * HALF_ROWS, LANES, dtype=bf16),
        in_specs=[pl.BlockSpec(memory_space=pl.ANY)],
        out_specs=VMEM,
        scratch_shapes=[
            pltpu.VMEM((ROWS + SPARE, 1, LANES), bf16),
            pltpu.SemaphoreType.DMA((len(STEPS),)),
            pltpu.VMEM((ROWS + SPARE, LANES), f32),
            pltpu.VMEM((NC * HALF_ROWS + SPARE, LANES), f32),
        ],
        compiler_params=pltpu.CompilerParams(vmem_limit_bytes=51 * 1024 * 1024),
    )(grads.reshape(ROWS, 1, LANES))


def cubes():
    def pair(k, parity, count, shifted):
        return (2 * k + 2 * shifted * (1 - parity) + parity) % count

    groups = []
    for c in range(NC):
        for kz in range(NZ // 2):
            for kx in range(NX // 2):
                for ky in range(NY // 2):
                    group = []
                    for label in range(N_CUBE):
                        z = pair(kz, label // 4, NZ, c)
                        x = pair(kx, label // 2 % 2, NX, c)
                        y = pair(ky, label % 2, NY, 1 - c)
                        group.append(((z * NX + x) * NC + c) * NY + y)
                    groups.append(group)
    return groups


def half_kernel(mine, r_ref, o_ref):
    c = lax.axis_index("c")
    c = c if mine else 1 - c
    at = pl.ds(pl.multiple_of(c * HALF_ROWS, 16), HALF_ROWS)
    total = r_ref[0, at, :].astype(f32)
    for k in range(1, N_CUBE):
        total = total + r_ref[k, at, :].astype(f32)
    o_ref[...] = total


def spread_kernel(a_ref, b_ref, o_ref, rows):
    rows[:HALF_ROWS, :] = a_ref[...] + b_ref[...]
    for k in range(N_WIDE):
        o_ref[k, :TOUCHED, :] = rows[k * TOUCHED : (k + 1) * TOUCHED, :]
        o_ref[k, TOUCHED:, :] = jnp.zeros((SLOT - TOUCHED, LANES), f32)


def slot_positions():
    q, y = q_index(), y_index()
    owner = (z_index() * NQ + q) * NY + y
    row = lax.broadcasted_iota(jnp.int32, (SLOT, LANES), 0)
    lane = lax.broadcasted_iota(jnp.int32, (SLOT, LANES), 1)
    local = row * LANES + lane - 2 * (NY * q + y)
    return local + owner * SHARD, (local >= 0) & (local < SHARD)


def in_layer(tab_ref, l, pos):
    start = tab_ref[l]
    return (pos >= start) & (pos < start + tab_ref[LAYERS + l])


def skipped(tab_ref, l):
    return tab_ref[2 * LAYERS + l].astype(f32)


def placed(flat_ref, rows):
    whole = SHARD // LANES
    rows[...] = jnp.zeros((SLOT + 8 + SPARE, LANES), f32)
    for k in range(whole):
        rows[8 + k, :] = flat_ref[pl.ds(k * LANES, LANES)]
    rows[8 + whole, pl.ds(0, SHARD - whole * LANES)] = flat_ref[pl.ds(whole * LANES, SHARD - whole * LANES)]
    shift = 2 * (NY * q_index() + y_index())
    lane = lax.broadcasted_iota(jnp.int32, (SLOT, LANES), 1)
    here = pltpu.roll(rows[8 : SLOT + 8, :], shift, 1)
    above = pltpu.roll(rows[7 : SLOT + 7, :], shift, 1)
    return jnp.where(lane >= shift, here, above)


def owner_kernel(tab_ref, r_ref, mf_ref, vf_ref, o_ref, h_ref, m_ref, v_ref, turn):
    m_ref[...] = placed(mf_ref, turn)
    v_ref[...] = placed(vf_ref, turn)
    g = r_ref[0]
    for k in range(1, N_WIDE):
        g = g + r_ref[k]
    pos, valid = slot_positions()
    g = jnp.where(valid, g * (1.0 / 512.0), 0.0)
    m = m_ref[...]
    row = lax.broadcasted_iota(jnp.int32, (SLOT, LANES), 0)
    lane = lax.broadcasted_iota(jnp.int32, (SLOT, LANES), 1)
    stack = jnp.zeros((SLOT, LANES), f32)
    decay = jnp.zeros((SLOT, LANES), f32)
    mm, gg = m * m, g * g
    for l in range(LAYERS):
        mask = in_layer(tab_ref, l, pos)
        decay = jnp.where(mask, (1.0 - skipped(tab_ref, l)) * 0.001, decay)
        for at, square in ((l, mm), (8 + l, gg)):
            rows = jnp.sum(jnp.where(mask, square, 0.0), axis=0, keepdims=True)
            stack = jnp.where(row == at, rows, stack)
    sums = jnp.sum(stack, axis=1, keepdims=True)
    total = jnp.sum(jnp.where(lane == row, sums, 0.0), axis=0, keepdims=True)
    h = g + decay * m
    h_ref[...] = h
    out = jnp.where(row == TOUCHED, total, h)
    a = m - 0.9 * v_ref[...]
    for k in range(N_FAR):
        o_ref[k, :SLOT, :] = out
        o_ref[k, SLOT:, :] = a


def group_kernel(s_ref, n_ref):
    total = s_ref[0, TOUCHED : TOUCHED + 1, :]
    for k in range(1, N_FAR):
        total = total + s_ref[k, TOUCHED : TOUCHED + 1, :]
    n_ref[...] = jnp.broadcast_to(total[None], n_ref.shape)


def trust_at(tab_ref, trust, pos):
    lane = lax.broadcasted_iota(jnp.int32, (1, LANES), 1)
    out = jnp.zeros(pos[0].shape, f32)
    outs = [out] * len(pos)
    for l in range(LAYERS):
        one = jnp.sum(jnp.where(lane == l, trust, 0.0), axis=1, keepdims=True)
        outs = [jnp.where(in_layer(tab_ref, l, p), one, o) for p, o in zip(pos, outs)]
    return outs


def update_kernel(tab_ref, n_ref, s_ref, w_ref, t_ref, rows):
    norms = jnp.sum(n_ref[...], axis=0)
    lane = lax.broadcasted_iota(jnp.int32, (1, LANES), 1)
    skip = jnp.zeros((1, LANES), f32)
    for l in range(LAYERS):
        skip = jnp.where(lane == l, skipped(tab_ref, l), skip)
    wnorm = jnp.sqrt(norms)
    gnorm = pltpu.roll(wnorm, LANES - 8, 1)
    ratio = 0.02 * wnorm / (gnorm + 0.001 * wnorm + 1e-06)
    trust = skip + (1.0 - skip) * ratio
    t_ref[...] = trust
    at = lax.broadcasted_iota(jnp.int32, (SLOT, LANES), 0) * LANES
    at = at + lax.broadcasted_iota(jnp.int32, (SLOT, LANES), 1)
    pos = [
        at + row_of(zh * NL + lax.axis_index("zl"), q_index(), yh * NL + lax.axis_index("yl")) * LANES
        for _, zh, yh in far_slots()
    ]
    for k, t in enumerate(trust_at(tab_ref, trust, pos)):
        w = s_ref[k, SLOT:, :] - 8.0 * t * s_ref[k, :SLOT, :]
        rows[k * TOUCHED : (k + 1) * TOUCHED, :] = w[:TOUCHED, :]
    w = rows[:NEAR_ROWS, :].astype(bf16)
    for k in range(NL * NX * NL):
        w_ref[k] = w


def own_kernel(tab_ref, t_ref, h_ref, m_ref, v_ref, om_ref, ov_ref, turn):
    shift = 2 * (NY * q_index() + y_index())
    pos, _ = slot_positions()
    (trust,) = trust_at(tab_ref, t_ref[...], [pos])
    new_v = 0.9 * v_ref[...] + 8.0 * trust * h_ref[...]
    new_m = m_ref[...] - new_v
    lane = lax.broadcasted_iota(jnp.int32, (SLOT, LANES), 1)
    for own, out in ((new_m, om_ref), (new_v, ov_ref)):
        turned = pltpu.roll(own, lax.rem(LANES - shift, LANES), 1)
        turn[:SLOT, :] = turned
        turn[SLOT:, :] = jnp.zeros((8, LANES), f32)
        out[...] = jnp.where(lane < LANES - shift, turned, turn[1 : SLOT + 1, :])


def put_core(w_ref, c, z, block, rows, tail):
    zh, zl = z // NL, z % NL
    part = NH * TOUCHED
    for x in range(NX):
        for yl in range(NL):
            peer = (zl * NX + x) * NL + yl
            block[yl * part : (yl + 1) * part, :] = w_ref[peer, zh * part : (zh + 1) * part, :].astype(f32)
        before = None
        for y in range(NY):
            at = (y % NL) * part + y // NL * TOUCHED
            base = row_of(z, x * NC, y) + c * Q_ROWS
            if before is None:
                rows[pl.ds(base, Y_ROWS), :] = block[at : at + Y_ROWS, :]
            else:
                rows[pl.ds(base, 1), :] = block[at : at + 1, :] + block[before : before + 1, :]
                rows[pl.ds(base + 1, Y_ROWS - 1), :] = block[at + 1 : at + Y_ROWS, :]
            before = at + Y_ROWS
        tail[pl.ds(z * NQ + x * NC + c, 1), :] = block[before : before + 1, :]


def own_half_kernel(w_ref, rows, tail, block):
    for z in range(NZ):
        put_core(w_ref, lax.axis_index("c"), z, block, rows, tail)


def lay_out_kernel(w_ref, rows_in, tail_in, rows, tail, o_ref, block, narrow, sems):
    copies = []
    for z in range(NZ):
        put_core(w_ref, 1 - lax.axis_index("c"), z, block, rows, tail)
        for q in range(NQ):
            last = row_of(z, q + 1, 0)
            one = tail[z * NQ + q : z * NQ + q + 1, :]
            if q + 1 < NQ:
                rows[last : last + 1, :] += one
            else:
                rows[last : last + 1, :] = one
        start, stop = z * Z_ROWS // 8 * 8, (z + 1) * Z_ROWS // 8 * 8
        narrow[start:stop, :] = rows[start:stop, :].astype(bf16)
        at = pl.ds(start, stop - start)
        copies.append(pltpu.make_async_copy(narrow.at[at], o_ref.at[at], sems.at[z]))
        copies[-1].start()
    for copy in copies:
        copy.wait()


def sent(x, axes):
    return lax.all_to_all(x, axes, 0, 0, tiled=True)


def swapped(x):
    return lax.ppermute(x, "c", [(0, 1), (1, 0)])


def shards(grads, master, velocity, layer_offsets, layer_sizes, lars_skip):
    tab = jnp.concatenate([layer_offsets, layer_sizes, lars_skip])
    near, far, slot = (NEAR_ROWS, LANES), (SLOT, LANES), shape(SLOT, LANES)
    sending, tab = lax.optimization_barrier((packed(grads), tab))
    received = lax.all_to_all(sending, AXES, 0, 0, axis_index_groups=cubes(), tiled=True)
    half = (HALF_ROWS, LANES)
    give = swapped(call(functools.partial(half_kernel, False), shape(*half), [VMEM])(received))
    keep = call(functools.partial(half_kernel, True), shape(*half), [VMEM])(received)
    spread = call(spread_kernel, shape(N_WIDE, *far), [VMEM, VMEM], [(HALF_ROWS + SPARE, LANES)])(keep, give)
    shared, h, m, v = call(
        owner_kernel,
        (shape(N_FAR, 2 * SLOT, LANES), slot, slot, slot),
        [SMEM] + [VMEM] * 3,
        [(SLOT + 8 + SPARE, LANES)],
    )(tab, sent(spread, WIDE), master, velocity)
    shared = sent(shared, FAR)
    norms = call(group_kernel, shape(N_NEAR, 1, LANES), [VMEM])(shared)
    w, trust = call(
        update_kernel,
        (shape(NL * NX * NL, *near, dtype=bf16), shape(1, LANES)),
        [SMEM, VMEM, VMEM],
        [(NEAR_ROWS + SPARE, LANES)],
    )(tab, sent(norms, NEAR), shared)
    w = sent(w, ("zl", "xh", "xl", "yl"))
    other = swapped(w)
    halves = (shape(ROWS + SPARE, LANES), shape(NZ * NQ + SPARE, LANES))
    block = (NL * NH * TOUCHED + SPARE, LANES)
    rows, tail = call(own_half_kernel, halves, [VMEM], [block])(w)
    new_master, new_velocity = call(
        own_kernel, (slot, slot), [SMEM] + [VMEM] * 4, [(SLOT + 8, LANES)]
    )(tab, trust, h, m, v)
    _, _, weights = pl.pallas_call(
        lay_out_kernel,
        out_shape=(*halves, shape(ROWS, LANES, dtype=bf16)),
        in_specs=[VMEM] * 3,
        out_specs=(VMEM, VMEM, pl.BlockSpec(memory_space=pl.ANY)),
        input_output_aliases={1: 0, 2: 1},
        scratch_shapes=[
            pltpu.VMEM(block, f32),
            pltpu.VMEM((ROWS, LANES), bf16),
            pltpu.SemaphoreType.DMA((NZ,)),
        ],
        compiler_params=PARAMS,
    )(other, rows, tail)
    return (
        weights.reshape(ROWS * LANES),
        new_master.reshape(SLOT * LANES)[:SHARD],
        new_velocity.reshape(SLOT * LANES)[:SHARD],
    )


def solution(mesh):
    finer = Mesh(mesh.devices.reshape(NH, NL, NXH, 2, NC, NH, NL), AXES)
    owned = P(AXES)
    in_specs = (P(("zh", "zl", "xh", "xl", "c"), ("yh", "yl"), None), owned, owned, P(), P(), P())
    return jax.shard_map(
        shards, mesh=finer, in_specs=in_specs, out_specs=(P(), owned, owned), check_vma=False
    )
```

```python
import functools

import jax
import jax.numpy as jnp
from jax import lax
from jax.experimental import pallas as pl
from jax.experimental.pallas import tpu as pltpu
from jax.sharding import Mesh
from jax.sharding import PartitionSpec as P

AXES = ("zh", "zl", "xh", "xl", "c", "yh", "yl")
NEAR = ("zl", "xh", "xl", "c", "yl")
FAR = ("zh", "yh")
WIDE = ("zh", "xh", "yh")
NX, NC, NL, NH = 4, 2, 2, 4
NY, NZ = NH * NL, NH * NL
NQ = NX * NC
N_NEAR, N_FAR = NL * NQ * NL, NH * NH
LANES = 128
SHARD = 1666
ROWS = 6664
Z_ROWS = ROWS // NZ
Q_ROWS = 104
Y_ROWS = 13
TOUCHED = 14
SLOT = 16
NEAR_ROWS = N_FAR * TOUCHED
NXH = NX // 2
N_CUBE, N_WIDE = 8, NH * NXH * NH
HALF_ROWS = N_WIDE * TOUCHED
LAYERS = 6
CHUNK = 136
STEPS = (2, 5, 7, 7, 7, 7, 7, 7)
SPARE = 8
f32 = jnp.float32
bf16 = jnp.bfloat16
VMEM = pl.BlockSpec(memory_space=pltpu.VMEM)
SMEM = pl.BlockSpec(memory_space=pltpu.SMEM)
PARAMS = pltpu.CompilerParams(vmem_limit_bytes=40 * 1024 * 1024)


def shape(*dims, dtype=f32):
    return jax.ShapeDtypeStruct(dims, dtype)


def call(kernel, out_shape, ins, scratch=()):
    many = isinstance(out_shape, tuple)
    return pl.pallas_call(
        kernel,
        out_shape=out_shape,
        in_specs=list(ins),
        out_specs=(VMEM,) * len(out_shape) if many else VMEM,
        scratch_shapes=[pltpu.VMEM(s, f32) for s in scratch],
        compiler_params=PARAMS,
    )


def row_of(z, q, y):
    return z * Z_ROWS + q * Q_ROWS + y * Y_ROWS


def z_index():
    return lax.axis_index("zh") * NL + lax.axis_index("zl")


def q_index():
    return (lax.axis_index("xh") * 2 + lax.axis_index("xl")) * NC + lax.axis_index("c")


def y_index():
    return lax.axis_index("yh") * NL + lax.axis_index("yl")


def far_slots():
    return [(k, k // NH, k % NH) for k in range(N_FAR)]


def pack_kernel(x_ref, o_ref, held, sems, wide, rows):
    copies, starts = [], [CHUNK * sum(STEPS[:i]) for i in range(len(STEPS))]
    for i, count in enumerate(STEPS):
        at = pl.ds(starts[i], count * CHUNK)
        copies.append(pltpu.make_async_copy(x_ref.at[at], held.at[at], sems.at[i]))
        copies[-1].start()
    for i, count in enumerate(STEPS):
        copies[i].wait()

        def widen(k, _):
            at = starts[i] + k * CHUNK
            for r in range(CHUNK):
                wide[pl.ds(at + r, 1), :] = held[at + r].astype(f32)
            return _

        lax.fori_loop(0, count, widen, 0)
    for label in range(N_CUBE):
        zl, xl, yl = label // 4, label // 2 % 2, label % 2
        for k in range(NC * N_WIDE):
            c, zh, xh, yh = k // N_WIDE, k // (NXH * NH) % NH, k // NH % NXH, k % NH
            base = row_of(zh * NL + zl, (xh * 2 + xl) * NC + c, yh * NL + yl)
            rows[k * TOUCHED : (k + 1) * TOUCHED, :] = wide[base : base + TOUCHED, :]
        o_ref[label] = rows[: NC * HALF_ROWS, :].astype(bf16)


def packed(grads):
    return pl.pallas_call(
        pack_kernel,
        out_shape=shape(N_CUBE, NC * HALF_ROWS, LANES, dtype=bf16),
        in_specs=[pl.BlockSpec(memory_space=pl.ANY)],
        out_specs=VMEM,
        scratch_shapes=[
            pltpu.VMEM((ROWS + SPARE, 1, LANES), bf16),
            pltpu.SemaphoreType.DMA((len(STEPS),)),
            pltpu.VMEM((ROWS + SPARE, LANES), f32),
            pltpu.VMEM((NC * HALF_ROWS + SPARE, LANES), f32),
        ],
        compiler_params=pltpu.CompilerParams(vmem_limit_bytes=51 * 1024 * 1024),
    )(grads.reshape(ROWS, 1, LANES))


def cubes():
    def pair(k, parity, count, shifted):
        return (2 * k + 2 * shifted * (1 - parity) + parity) % count

    groups = []
    for c in range(NC):
        for kz in range(NZ // 2):
            for kx in range(NX // 2):
                for ky in range(NY // 2):
                    group = []
                    for label in range(N_CUBE):
                        z = pair(kz, label // 4, NZ, c)
                        x = pair(kx, label // 2 % 2, NX, c)
                        y = pair(ky, label % 2, NY, 1 - c)
                        group.append(((z * NX + x) * NC + c) * NY + y)
                    groups.append(group)
    return groups


def half_kernel(mine, r_ref, o_ref):
    c = lax.axis_index("c")
    c = c if mine else 1 - c
    at = pl.ds(pl.multiple_of(c * HALF_ROWS, 16), HALF_ROWS)
    total = r_ref[0, at, :].astype(f32)
    for k in range(1, N_CUBE):
        total = total + r_ref[k, at, :].astype(f32)
    o_ref[...] = total


def spread_kernel(a_ref, b_ref, o_ref, rows):
    rows[:HALF_ROWS, :] = a_ref[...] + b_ref[...]
    for k in range(N_WIDE):
        for r in range(TOUCHED):
            at = k * TOUCHED + r
            o_ref[k, :, r * LANES : (r + 1) * LANES] = rows[at : at + 1, :]


def slot_positions():
    q, y = q_index(), y_index()
    owner = (z_index() * NQ + q) * NY + y
    row = lax.broadcasted_iota(jnp.int32, (SLOT, LANES), 0)
    lane = lax.broadcasted_iota(jnp.int32, (SLOT, LANES), 1)
    local = row * LANES + lane - 2 * (NY * q + y)
    return local + owner * SHARD, (local >= 0) & (local < SHARD)


def in_layer(tab_ref, l, pos):
    start = tab_ref[l]
    return (pos >= start) & (pos < start + tab_ref[LAYERS + l])


def skipped(tab_ref, l):
    return tab_ref[2 * LAYERS + l].astype(f32)


def placed(flat_ref, rows):
    whole = SHARD // LANES
    rows[...] = jnp.zeros((SLOT + 8 + SPARE, LANES), f32)
    for k in range(whole):
        rows[8 + k, :] = flat_ref[pl.ds(k * LANES, LANES)]
    rows[8 + whole, pl.ds(0, SHARD - whole * LANES)] = flat_ref[pl.ds(whole * LANES, SHARD - whole * LANES)]
    shift = 2 * (NY * q_index() + y_index())
    lane = lax.broadcasted_iota(jnp.int32, (SLOT, LANES), 1)
    here = pltpu.roll(rows[8 : SLOT + 8, :], shift, 1)
    above = pltpu.roll(rows[7 : SLOT + 7, :], shift, 1)
    return jnp.where(lane >= shift, here, above)


def owner_kernel(tab_ref, r_ref, mf_ref, vf_ref, o_ref, h_ref, m_ref, v_ref, turn):
    m_ref[...] = placed(mf_ref, turn)
    v_ref[...] = placed(vf_ref, turn)
    flat = r_ref[0]
    for k in range(1, N_WIDE):
        flat = flat + r_ref[k]
    turn[TOUCHED:SLOT, :] = jnp.zeros((SLOT - TOUCHED, LANES), f32)
    for r in range(TOUCHED):
        turn[r : r + 1, :] = flat[:, r * LANES : (r + 1) * LANES]
    g = turn[:SLOT, :]
    pos, valid = slot_positions()
    g = jnp.where(valid, g * (1.0 / 512.0), 0.0)
    m = m_ref[...]
    row = lax.broadcasted_iota(jnp.int32, (SLOT, LANES), 0)
    lane = lax.broadcasted_iota(jnp.int32, (SLOT, LANES), 1)
    stack = jnp.zeros((SLOT, LANES), f32)
    decay = jnp.zeros((SLOT, LANES), f32)
    mm, gg = m * m, g * g
    for l in range(LAYERS):
        mask = in_layer(tab_ref, l, pos)
        decay = jnp.where(mask, (1.0 - skipped(tab_ref, l)) * 0.001, decay)
        for at, square in ((l, mm), (8 + l, gg)):
            rows = jnp.sum(jnp.where(mask, square, 0.0), axis=0, keepdims=True)
            stack = jnp.where(row == at, rows, stack)
    sums = jnp.sum(stack, axis=1, keepdims=True)
    total = jnp.sum(jnp.where(lane == row, sums, 0.0), axis=0, keepdims=True)
    h = g + decay * m
    h_ref[...] = h
    out = jnp.where(row == TOUCHED, total, h)
    a = m - 0.9 * v_ref[...]
    for k in range(N_FAR):
        o_ref[k, :SLOT, :] = out
        o_ref[k, SLOT:, :] = a


def group_kernel(s_ref, n_ref):
    total = s_ref[0, TOUCHED : TOUCHED + 1, :]
    for k in range(1, N_FAR):
        total = total + s_ref[k, TOUCHED : TOUCHED + 1, :]
    n_ref[...] = jnp.broadcast_to(total[None], n_ref.shape)


def trust_at(tab_ref, trust, pos):
    lane = lax.broadcasted_iota(jnp.int32, (1, LANES), 1)
    out = jnp.zeros(pos[0].shape, f32)
    outs = [out] * len(pos)
    for l in range(LAYERS):
        one = jnp.sum(jnp.where(lane == l, trust, 0.0), axis=1, keepdims=True)
        outs = [jnp.where(in_layer(tab_ref, l, p), one, o) for p, o in zip(pos, outs)]
    return outs


def update_kernel(tab_ref, n_ref, s_ref, w_ref, t_ref, rows):
    norms = jnp.sum(n_ref[...], axis=0)
    lane = lax.broadcasted_iota(jnp.int32, (1, LANES), 1)
    skip = jnp.zeros((1, LANES), f32)
    for l in range(LAYERS):
        skip = jnp.where(lane == l, skipped(tab_ref, l), skip)
    wnorm = jnp.sqrt(norms)
    gnorm = pltpu.roll(wnorm, LANES - 8, 1)
    ratio = 0.02 * wnorm / (gnorm + 0.001 * wnorm + 1e-06)
    trust = skip + (1.0 - skip) * ratio
    t_ref[...] = trust
    at = lax.broadcasted_iota(jnp.int32, (SLOT, LANES), 0) * LANES
    at = at + lax.broadcasted_iota(jnp.int32, (SLOT, LANES), 1)
    pos = [
        at + row_of(zh * NL + lax.axis_index("zl"), q_index(), yh * NL + lax.axis_index("yl")) * LANES
        for _, zh, yh in far_slots()
    ]
    for k, t in enumerate(trust_at(tab_ref, trust, pos)):
        w = s_ref[k, SLOT:, :] - 8.0 * t * s_ref[k, :SLOT, :]
        rows[k * TOUCHED : (k + 1) * TOUCHED, :] = w[:TOUCHED, :]
    w = rows[:NEAR_ROWS, :].astype(bf16)
    for k in range(NL * NX * NL):
        w_ref[k] = w


def own_kernel(tab_ref, t_ref, h_ref, m_ref, v_ref, om_ref, ov_ref, turn):
    shift = 2 * (NY * q_index() + y_index())
    pos, _ = slot_positions()
    (trust,) = trust_at(tab_ref, t_ref[...], [pos])
    new_v = 0.9 * v_ref[...] + 8.0 * trust * h_ref[...]
    new_m = m_ref[...] - new_v
    lane = lax.broadcasted_iota(jnp.int32, (SLOT, LANES), 1)
    for own, out in ((new_m, om_ref), (new_v, ov_ref)):
        turned = pltpu.roll(own, lax.rem(LANES - shift, LANES), 1)
        turn[:SLOT, :] = turned
        turn[SLOT:, :] = jnp.zeros((8, LANES), f32)
        out[...] = jnp.where(lane < LANES - shift, turned, turn[1 : SLOT + 1, :])


def put_core(w_ref, c, z, block, rows, tail):
    zh, zl = z // NL, z % NL
    part = NH * TOUCHED
    for x in range(NX):
        for yl in range(NL):
            peer = (zl * NX + x) * NL + yl
            block[yl * part : (yl + 1) * part, :] = w_ref[peer, zh * part : (zh + 1) * part, :].astype(f32)
        before = None
        for y in range(NY):
            at = (y % NL) * part + y // NL * TOUCHED
            base = row_of(z, x * NC, y) + c * Q_ROWS
            if before is None:
                rows[pl.ds(base, Y_ROWS), :] = block[at : at + Y_ROWS, :]
            else:
                rows[pl.ds(base, 1), :] = block[at : at + 1, :] + block[before : before + 1, :]
                rows[pl.ds(base + 1, Y_ROWS - 1), :] = block[at + 1 : at + Y_ROWS, :]
            before = at + Y_ROWS
        tail[pl.ds(z * NQ + x * NC + c, 1), :] = block[before : before + 1, :]


def own_half_kernel(w_ref, rows, tail, block):
    for z in range(NZ):
        put_core(w_ref, lax.axis_index("c"), z, block, rows, tail)


def lay_out_kernel(w_ref, rows_in, tail_in, rows, tail, o_ref, block, narrow, sems):
    copies = []
    for z in range(NZ):
        put_core(w_ref, 1 - lax.axis_index("c"), z, block, rows, tail)
        for q in range(NQ):
            last = row_of(z, q + 1, 0)
            one = tail[z * NQ + q : z * NQ + q + 1, :]
            if q + 1 < NQ:
                rows[last : last + 1, :] += one
            else:
                rows[last : last + 1, :] = one
        start, stop = z * Z_ROWS // 8 * 8, (z + 1) * Z_ROWS // 8 * 8
        narrow[start:stop, :] = rows[start:stop, :].astype(bf16)
        at = pl.ds(start, stop - start)
        copies.append(pltpu.make_async_copy(narrow.at[at], o_ref.at[at], sems.at[z]))
        copies[-1].start()
    for copy in copies:
        copy.wait()


def sent(x, axes):
    return lax.all_to_all(x, axes, 0, 0, tiled=True)


def swapped(x):
    return lax.ppermute(x, "c", [(0, 1), (1, 0)])


def shards(grads, master, velocity, layer_offsets, layer_sizes, lars_skip):
    tab = jnp.concatenate([layer_offsets, layer_sizes, lars_skip])
    near, slot = (NEAR_ROWS, LANES), shape(SLOT, LANES)
    sending, tab = lax.optimization_barrier((packed(grads), tab))
    received = lax.all_to_all(sending, AXES, 0, 0, axis_index_groups=cubes(), tiled=True)
    half = (HALF_ROWS, LANES)
    give = swapped(call(functools.partial(half_kernel, False), shape(*half), [VMEM])(received))
    keep = call(functools.partial(half_kernel, True), shape(*half), [VMEM])(received)
    spread = call(spread_kernel, shape(N_WIDE, 1, TOUCHED * LANES), [VMEM, VMEM], [(HALF_ROWS + SPARE, LANES)])(keep, give)
    shared, h, m, v = call(
        owner_kernel,
        (shape(N_FAR, 2 * SLOT, LANES), slot, slot, slot),
        [SMEM] + [VMEM] * 3,
        [(SLOT + 8 + SPARE, LANES)],
    )(tab, sent(spread, WIDE), master, velocity)
    shared = sent(shared, FAR)
    norms = call(group_kernel, shape(N_NEAR, 1, LANES), [VMEM])(shared)
    w, trust = call(
        update_kernel,
        (shape(NL * NX * NL, *near, dtype=bf16), shape(1, LANES)),
        [SMEM, VMEM, VMEM],
        [(NEAR_ROWS + SPARE, LANES)],
    )(tab, sent(norms, NEAR), shared)
    w = sent(w, ("zl", "xh", "xl", "yl"))
    other = swapped(w)
    halves = (shape(ROWS + SPARE, LANES), shape(NZ * NQ + SPARE, LANES))
    block = (NL * NH * TOUCHED + SPARE, LANES)
    rows, tail = call(own_half_kernel, halves, [VMEM], [block])(w)
    new_master, new_velocity = call(
        own_kernel, (slot, slot), [SMEM] + [VMEM] * 4, [(SLOT + 8, LANES)]
    )(tab, trust, h, m, v)
    _, _, weights = pl.pallas_call(
        lay_out_kernel,
        out_shape=(*halves, shape(ROWS, LANES, dtype=bf16)),
        in_specs=[VMEM] * 3,
        out_specs=(VMEM, VMEM, pl.BlockSpec(memory_space=pl.ANY)),
        input_output_aliases={1: 0, 2: 1},
        scratch_shapes=[
            pltpu.VMEM(block, f32),
            pltpu.VMEM((ROWS, LANES), bf16),
            pltpu.SemaphoreType.DMA((NZ,)),
        ],
        compiler_params=PARAMS,
    )(other, rows, tail)
    return (
        weights.reshape(ROWS * LANES),
        new_master.reshape(SLOT * LANES)[:SHARD],
        new_velocity.reshape(SLOT * LANES)[:SHARD],
    )


def solution(mesh):
    finer = Mesh(mesh.devices.reshape(NH, NL, NXH, 2, NC, NH, NL), AXES)
    owned = P(AXES)
    in_specs = (P(("zh", "zl", "xh", "xl", "c"), ("yh", "yl"), None), owned, owned, P(), P(), P())
    return jax.shard_map(
        shards, mesh=finer, in_specs=in_specs, out_specs=(P(), owned, owned), check_vma=False
    )
```
